256 devices in a mesh: row: 32 (over y, x, core), col: 8 (over z).
Axes of the slice: x: 4, y: 4, z: 8, core: 2. Of those that a mesh axis runs over, the one named last changes fastest.
Arguments:
- covariance: bfloat16 [16384, 16384], P('row', 'col'), may hold values from -0.12 to 0.6, as said below
- estimate: bfloat16 [16384, 16384], P('row', 'col'), may hold values from -2.3 to 12, as said below
- dual_var: bfloat16 [16384, 16384], P('row', 'col'), may hold values from -1.7 to 1.7, as said below
- start_basis: float32 [16384, 128], P('row'), may hold values from -6 to 6
Outputs:
- next_estimate: float32 [16384, 16384], P('row', 'col')
- next_dual: bfloat16 [16384, 16384], P('row', 'col')
The draws below stay inside these ranges and needn't reach their ends.
Inputs may be any that keep to these rules, and one draw needn't show every extreme that they name: `covariance`: symmetric. `estimate`: symmetric. `dual_var`: symmetric.
All inputs are finite; a program needn't handle non-finite values.
Results may differ from the reference program's by a relative error of at most 0.001.
Values sent between devices are 32-bit elements; how exact they have to be, the bound alone decides.
A program may use at most 64 MiB of HBM per device.

```python
import jax
import jax.numpy as jnp
from jax import lax

P_SIZE = 16384
RANK = 128
ITERS = 1
NS_ITERS = 12
N_ROW = 32


def symmetric_part(key, spread):
    raw_draw = jax.random.truncated_normal(key, -4.0, 4.0, (P_SIZE, P_SIZE), jnp.float32)
    return (raw_draw + raw_draw.T) * (spread * 0.7071067811865476)


def on_diagonal():
    row_ids = lax.broadcasted_iota(jnp.int32, (P_SIZE, 1), 0)
    col_ids = lax.broadcasted_iota(jnp.int32, (1, P_SIZE), 1)
    return row_ids == col_ids


def draw_covariance(key, part):
    off_diag = symmetric_part(jax.random.fold_in(key, 11), 0.005)
    variances = jax.random.uniform(jax.random.fold_in(key, 12), (P_SIZE,), jnp.float32, 0.05, 0.15)
    matrix = jnp.where(on_diagonal(), variances[:, None], off_diag)
    return matrix.astype(jnp.bfloat16)


def draw_estimate(key, part):
    off_diag = symmetric_part(jax.random.fold_in(key, 21), 0.4)
    diagonal = jax.random.uniform(jax.random.fold_in(key, 22), (P_SIZE,), jnp.float32, 8.0, 12.0)
    return jnp.where(on_diagonal(), diagonal[:, None], off_diag).astype(jnp.bfloat16)


def draw_dual_var(key, part):
    return symmetric_part(jax.random.fold_in(key, 31), 0.3).astype(jnp.bfloat16)


def steps_of(stream_key, shape, split, least, top_value):
    def one(dim, blocks):
        steps = jax.random.uniform(jax.random.fold_in(jax.random.fold_in(stream_key, 6), dim), (blocks,), jnp.float32, least / len(split), top_value / len(split))
        return jnp.repeat(jnp.exp(steps), shape[dim] // blocks).reshape((-1,) + (1,) * (len(shape) - dim - 1))

    gain = one(*split[0])
    for cut in split[1:]:
        gain = gain * one(*cut)
    return gain


def bell_draw(stream_key, extent, scale, limit, cuts=(), kind=jnp.bfloat16):
    array = scale * jax.random.normal(stream_key, extent, jnp.float32)
    if cuts:
        array = array * steps_of(stream_key, extent, cuts, -0.22, 0.18)
    return jnp.clip(array, -limit, limit).astype(kind)


def setup_inputs(seed: int = 0) -> dict:
    keys = jax.random.split(jax.random.key(seed), 5)
    return {
        "covariance": draw_covariance(jax.random.fold_in(keys[4], 71), 0),
        "estimate": draw_estimate(jax.random.fold_in(keys[4], 71), 0),
        "dual_var": draw_dual_var(jax.random.fold_in(keys[4], 71), 0),
        "start_basis": bell_draw(keys[3], (P_SIZE, RANK), 1.0, 6.0, ((0, 32),), jnp.float32),
    }


penalty = 0.01
threshold = 0.2
base_level = 10.0
highest = lax.Precision.HIGHEST

def inner_product(left_side, right_side):
    return lax.dot_general(left_side.astype(jnp.float32), right_side.astype(jnp.float32), (((0,), (0,)), ((), ())), precision=highest, preferred_element_type=jnp.float32)

def normalize(mapped, gram_matrix):
    lower_factor = jnp.linalg.cholesky(gram_matrix)
    identity = jnp.eye(gram_matrix.shape[0], dtype=jnp.float32)
    inverse = lax.linalg.triangular_solve(lower_factor, identity, left_side=True, lower=True)
    return jnp.dot(mapped.astype(jnp.float32), inverse.T.astype(jnp.float32), precision=highest, preferred_element_type=jnp.float32)

def response_of(ritz_matrix):
    identity = jnp.eye(ritz_matrix.shape[0], dtype=jnp.float32)
    square = jnp.dot(ritz_matrix.astype(jnp.float32), ritz_matrix.astype(jnp.float32), precision=highest, preferred_element_type=jnp.float32) + 4.0 * penalty * identity
    frobenius = jnp.sqrt(jnp.sum(square * square))

    def newton(sweep_index, state_pair):
        iterate, partner = state_pair
        factor = 0.5 * (3.0 * identity - jnp.dot(partner.astype(jnp.float32), iterate.astype(jnp.float32), precision=highest, preferred_element_type=jnp.float32))
        return (jnp.dot(iterate.astype(jnp.float32), factor.astype(jnp.float32), precision=highest, preferred_element_type=jnp.float32), jnp.dot(factor.astype(jnp.float32), partner.astype(jnp.float32), precision=highest, preferred_element_type=jnp.float32))
    iterate, partner = lax.fori_loop(0, NS_ITERS, newton, (square / frobenius, identity))
    square_root = jnp.sqrt(frobenius) * iterate
    return (ritz_matrix + square_root) / (2.0 * penalty) - base_level * identity

def reference(covariance, estimate, dual_var, start_basis):
    shifted = penalty * (estimate.astype(jnp.float32) - dual_var.astype(jnp.float32)) - covariance.astype(jnp.float32)
    current = start_basis
    for sweep_index in range(ITERS):
        mapped = jnp.dot(shifted.astype(jnp.float32), current.astype(jnp.float32), precision=highest, preferred_element_type=jnp.float32)
        current = normalize(mapped, inner_product(mapped, mapped))
    product = jnp.dot(shifted.astype(jnp.float32), current.astype(jnp.float32), precision=highest, preferred_element_type=jnp.float32)
    raw_ritz = inner_product(current, product)
    ritz_matrix = 0.5 * (raw_ritz + raw_ritz.T)
    response = response_of(ritz_matrix)
    weighted = jnp.dot(current.astype(jnp.float32), response.astype(jnp.float32), precision=highest, preferred_element_type=jnp.float32)
    rows_block = P_SIZE // N_ROW

    def finish(block_index):
        row_start = block_index * rows_block
        left_rows = lax.dynamic_slice_in_dim(weighted, row_start, rows_block, 0)
        theta_tile = lax.dot_general(left_rows.astype(jnp.float32), current.astype(jnp.float32), (((1,), (1,)), ((), ())), precision=highest, preferred_element_type=jnp.float32)
        row_ids = row_start + lax.broadcasted_iota(jnp.int32, (rows_block, 1), 0)
        col_ids = lax.broadcasted_iota(jnp.int32, (1, P_SIZE), 1)
        theta_tile = theta_tile + jnp.where(row_ids == col_ids, base_level, 0.0)
        dual_rows = lax.dynamic_slice_in_dim(dual_var, row_start, rows_block, 0)
        mixture = theta_tile + dual_rows.astype(jnp.float32)
        clipped = jnp.clip(mixture, -threshold, threshold)
        return (mixture - clipped, clipped.astype(jnp.bfloat16))
    new_estimate, new_dual = lax.map(finish, jnp.arange(N_ROW, dtype=jnp.int32))
    return (new_estimate.reshape(P_SIZE, P_SIZE), new_dual.reshape(P_SIZE, P_SIZE))
```

```python
import functools

import jax
import jax.numpy as jnp
from jax import lax
from jax.experimental import pallas as pl
from jax.experimental.pallas import tpu as pltpu
from jax.sharding import PartitionSpec as P

NS_ITERS = 12
MESH = pl.DeviceIdType.MESH
F32 = jnp.float32
BF16 = jnp.bfloat16

penalty = 0.01
threshold = 0.2
base_level = 10.0
highest = lax.Precision.HIGHEST

NN = (((1,), (0,)), ((), ()))
NT = (((1,), (1,)), ((), ()))
TN = (((0,), (0,)), ((), ()))

PLANE = 16
DEPTH = 8
CHUNK = 64


def dot(left, right, dims=NN):
    return lax.dot_general(left, right, dims, preferred_element_type=F32)


def dot_full(left, right, dims=NN):
    return lax.dot_general(left, right, dims, precision=highest, preferred_element_type=F32)


def split(array):
    high = array.astype(BF16)
    return high, (array - high.astype(F32)).astype(BF16)


def dot_split(left, right, dims=NN):
    left_high, left_low = split(left)
    right_high, right_low = split(right)
    return dot(left_high, right_high, dims) + (
        dot(left_low, right_high, dims) + dot(left_high, right_low, dims)
    )


def loop(low, high, body):
    def step(index, carry):
        body(index)
        return carry

    lax.fori_loop(low, high, step, 0)


def solve_kernel(
    cov_hbm,
    est_hbm,
    dual_hbm,
    basis,
    left_out,
    right_out,
    cov,
    est,
    dual,
    a_high,
    a_low,
    part_other,
    part_own,
    half_in,
    rs_send,
    rs_in,
    image,
    z_in,
    rows_in,
    product,
    red_part,
    red_in,
    red_mid,
    red_mid_in,
    red_out,
    table,
    pair,
    load_sem,
    half_send,
    half_recv,
    rs_ssem,
    rs_rsem,
    ag_ssem,
    ag_rsem,
    fwd_send,
    fwd_recv,
    z_ssem,
    z_rsem,
    rows_ssem,
    rows_rsem,
    a_ssem,
    a_rsem,
    b_ssem,
    b_rsem,
    c_ssem,
    c_rsem,
):
    row = lax.axis_index("row")
    col = lax.axis_index("col")
    core = lax.rem(row, 2)
    chip = lax.div(row, 2)
    other = row + 1 - 2 * core
    own_chunk = core * PLANE + chip

    half = a_high.shape[1] // 2

    def load(index, side):
        source, target = ((cov_hbm, cov), (est_hbm, est), (dual_hbm, dual))[index]
        offset = pl.multiple_of((1 - core if side == 0 else core) * half, half)
        window = pl.ds(offset, half)
        return pltpu.make_async_copy(
            source.at[:, window], target.at[:, window], load_sem.at[index, side]
        )

    for side in range(2):
        for index in range(3):
            load(index, side).start()

    def plane_row(offset):
        return 2 * lax.rem(chip + offset, PLANE) + core

    def column_device(offset):
        target = lax.rem(2 * col + core + offset, 2 * DEPTH)
        return (2 * chip + lax.rem(target, 2), lax.div(target, 2))

    def rows_source(index):
        chunk = 8 * lax.rem(row, 4) + index
        return 2 * lax.rem(chunk, PLANE) + lax.div(chunk, PLANE)

    def rows_target(index):
        return 4 * index + lax.div(own_chunk, 8)

    barrier = pltpu.get_barrier_semaphore()

    def signal(device):
        pl.semaphore_signal(barrier, inc=1, device_id=device, device_id_type=MESH)

    loop(1, PLANE, lambda d: signal((plane_row(d), col)))
    loop(1, 2 * DEPTH, lambda d: signal(column_device(d)))

    def signal_source(index):
        source = rows_source(index)

        @pl.when(source != row)
        def _():
            signal((source, col))

    loop(0, 8, signal_source)

    has_own = lax.rem(row, 4) == lax.div(own_chunk, 8)
    peers = PLANE - 1 + 2 * DEPTH - 1 + 8 - jnp.where(has_own, 1, 0)

    flipped = basis[...].T
    flip_high, flip_low = split(flipped)
    flip_both = jnp.concatenate([flip_high, flip_low], axis=0)
    width = 256
    rank = flipped.shape[0]

    def partial_terms(side, target):
        offset = (1 - core if side == 0 else core) * half

        def block(index):
            window = pl.ds(pl.multiple_of(offset + index * width, width), width)
            shifted = penalty * (
                est[:, window].astype(F32) - dual[:, window].astype(F32)
            ) - cov[:, window].astype(F32)
            high, low = split(shifted)
            a_high[:, window] = high
            a_low[:, window] = low
            both = dot(flip_both, high)
            terms = both[:rank] + both[rank:] + dot(flip_high, low)
            pieces = width // CHUNK
            target[pl.ds(pieces * index, pieces)] = terms.T.reshape(pieces, CHUNK, rank)

        loop(0, half // width, block)

    for index in range(3):
        load(index, 0).wait()
    partial_terms(0, part_other)

    pl.semaphore_wait(barrier, peers)

    half_copy = pltpu.make_async_remote_copy(
        src_ref=part_other,
        dst_ref=half_in,
        send_sem=half_send,
        recv_sem=half_recv,
        device_id=(other, col),
        device_id_type=MESH,
    )
    half_copy.start()
    for index in range(3):
        load(index, 1).wait()
    partial_terms(1, part_own)
    half_copy.wait_recv()
    rs_send[...] = part_own[...] + half_in[...]

    def rs_copy(d):
        return pltpu.make_async_remote_copy(
            src_ref=rs_send.at[lax.rem(chip + d, PLANE)],
            dst_ref=rs_in.at[d],
            send_sem=rs_ssem.at[d],
            recv_sem=rs_rsem.at[d],
            device_id=(plane_row(d), col),
            device_id_type=MESH,
        )

    loop(1, PLANE, lambda d: rs_copy(d).start())
    total = rs_send[chip]
    loop(1, PLANE, lambda d: rs_copy(d).wait_recv())
    for d in range(1, PLANE):
        total = total + rs_in[d]
    image[own_chunk] = total
    z_in[col] = total

    def z_copy(d):
        return pltpu.make_async_remote_copy(
            src_ref=image.at[own_chunk],
            dst_ref=z_in.at[col],
            send_sem=z_ssem.at[d],
            recv_sem=z_rsem.at[d],
            device_id=(row, lax.rem(col + d, DEPTH)),
            device_id_type=MESH,
        )

    def ag_copy(d):
        return pltpu.make_async_remote_copy(
            src_ref=image.at[own_chunk],
            dst_ref=image.at[own_chunk],
            send_sem=ag_ssem.at[d],
            recv_sem=ag_rsem.at[d],
            device_id=(plane_row(d), col),
            device_id_type=MESH,
        )

    loop(1, DEPTH, lambda d: z_copy(d).start())
    loop(1, PLANE, lambda d: ag_copy(d).start())

    def a_copy(which, d):
        return pltpu.make_async_remote_copy(
            src_ref=red_part.at[which, lax.rem(chip + d, PLANE)],
            dst_ref=red_in.at[which, d],
            send_sem=a_ssem.at[which, d],
            recv_sem=a_rsem.at[which, d],
            device_id=(plane_row(d), col),
            device_id_type=MESH,
        )

    def b_copy(which, d):
        return pltpu.make_async_remote_copy(
            src_ref=red_mid.at[which],
            dst_ref=red_mid_in.at[which, d],
            send_sem=b_ssem.at[which, d],
            recv_sem=b_rsem.at[which, d],
            device_id=column_device(d),
            device_id_type=MESH,
        )

    def c_copy(which, d):
        return pltpu.make_async_remote_copy(
            src_ref=red_out.at[which, chip],
            dst_ref=red_out.at[which, chip],
            send_sem=c_ssem.at[which, d],
            recv_sem=c_rsem.at[which, d],
            device_id=(plane_row(d), col),
            device_id_type=MESH,
        )

    def reduce_start(which, value):
        red_part[which] = value.reshape(PLANE, 8, rank)
        loop(1, PLANE, lambda d: a_copy(which, d).start())

    def reduce_middle(which):
        loop(1, PLANE, lambda d: a_copy(which, d).wait_recv())
        piece = red_part[which, chip]
        for d in range(1, PLANE):
            piece = piece + red_in[which, d]
        red_mid[which] = piece
        loop(1, 2 * DEPTH, lambda d: b_copy(which, d).start())

    def reduce_spread(which):
        loop(1, 2 * DEPTH, lambda d: b_copy(which, d).wait_recv())
        piece = red_mid[which]
        for d in range(1, 2 * DEPTH):
            piece = piece + red_mid_in[which, d]
        red_out[which, chip] = piece
        loop(1, PLANE, lambda d: c_copy(which, d).start())

    def reduce_end(which):
        loop(1, PLANE, lambda d: c_copy(which, d).wait_recv())
        return red_out[which].reshape(rank, rank)

    reduce_start(0, dot_full(total, total, TN))

    loop(1, DEPTH, lambda d: z_copy(d).wait_recv())
    slot = lax.rem(own_chunk, 8)

    def rows_copy(index):
        return pltpu.make_async_remote_copy(
            src_ref=z_in.at[index],
            dst_ref=rows_in.at[slot],
            send_sem=rows_ssem.at[index],
            recv_sem=rows_rsem.at[slot],
            device_id=(rows_target(index), col),
            device_id_type=MESH,
        )

    def rows_start(index):
        @pl.when(rows_target(index) != row)
        def _():
            rows_copy(index).start()

        @pl.when(rows_target(index) == row)
        def _():
            rows_in[slot] = z_in[index]

    loop(0, DEPTH, rows_start)

    loop(1, PLANE, lambda d: ag_copy(d).wait_recv())
    own_half = image.at[pl.ds(core * PLANE, PLANE)]
    fwd_copy = pltpu.make_async_remote_copy(
        src_ref=own_half,
        dst_ref=own_half,
        send_sem=fwd_send,
        recv_sem=fwd_recv,
        device_id=(other, col),
        device_id_type=MESH,
    )
    fwd_copy.start()
    reduce_middle(0)
    fwd_copy.wait_recv()

    columns = image.shape[0] * CHUNK

    def split_block(index):
        values = image[pl.ds(4 * index, 4)].reshape(4 * CHUNK, rank)
        high, low = split(values)
        window = pl.ds(pl.multiple_of(4 * CHUNK * index, 4 * CHUNK), 4 * CHUNK)
        right_out[window, 0:rank] = high
        right_out[window, rank : 2 * rank] = low
        right_out[window, 2 * rank : 3 * rank] = high

    loop(0, columns // (4 * CHUNK), split_block)

    def product_block(index):
        window = pl.ds(pl.multiple_of(256 * index, 256), 256)
        both = dot(a_high[window, :], right_out[:, 0 : 2 * rank])
        product[window, :] = (
            both[:, :rank] + both[:, rank:] + dot(a_low[window, :], right_out[:, 0:rank])
        )

    loop(0, product.shape[0] // 256, product_block)
    reduce_spread(0)

    def rows_wait(index):
        @pl.when(rows_source(index) != row)
        def _():
            pltpu.make_async_remote_copy(
                src_ref=z_in.at[index],
                dst_ref=rows_in.at[index],
                send_sem=rows_ssem.at[index],
                recv_sem=rows_rsem.at[index],
                device_id=(rows_source(index), col),
                device_id_type=MESH,
            ).wait_recv()

    loop(0, 8, rows_wait)
    row_image = rows_in[...].reshape(8 * CHUNK, rank)
    reduce_start(1, dot_split(row_image, product[...], TN))

    row_ids = lax.broadcasted_iota(jnp.int32, (rank, rank), 0)
    col_ids = lax.broadcasted_iota(jnp.int32, (rank, rank), 1)
    identity = jnp.where(row_ids == col_ids, 1.0, 0.0).astype(F32)
    gram = reduce_end(0)
    table[:, :rank] = gram
    table[:, rank:] = identity

    def eliminate(step):
        pivot_row = table[pl.ds(step, 1), :]
        left_part = table[:, :rank]
        column = jnp.sum(jnp.where(col_ids == step, left_part, 0.0), axis=1, keepdims=True)
        pivot = jnp.sum(
            jnp.where(col_ids[:1] == step, pivot_row[:, :rank], 0.0), axis=1, keepdims=True
        )
        factor = jnp.where(row_ids[:, :1] > step, column / pivot, 0.0)
        table[...] = table[...] - factor * pivot_row

    loop(0, 44, eliminate)
    reduce_middle(1)
    loop(44, 86, eliminate)
    reduce_spread(1)
    loop(86, rank, eliminate)
    pivots = jnp.sum(table[:, :rank] * identity, axis=1, keepdims=True)
    inverse = table[:, rank:] / jnp.sqrt(pivots)

    inner = reduce_end(1)
    raw_ritz = dot_full(dot_full(inverse, inner), inverse, NT)
    ritz = 0.5 * (raw_ritz + raw_ritz.T)
    square = dot_full(ritz, ritz) + 4.0 * penalty * identity
    frobenius = jnp.sqrt(jnp.sum(square * square, keepdims=True))

    pair[0:rank] = square / frobenius
    pair[rank:] = identity

    def newton(step):
        factor = 0.5 * (3.0 * identity - dot_split(pair[rank:], pair[0:rank]))
        pair[...] = dot_split(pair[...], factor)

    loop(0, NS_ITERS, newton)
    iterate = pair[0:rank]
    response = (ritz + jnp.sqrt(frobenius) * iterate) / (2.0 * penalty) - base_level * identity
    core_matrix = dot_full(dot_full(inverse, response, TN), inverse)
    weighted_high, weighted_low = split(dot_split(row_image, core_matrix))
    left_out[:, 0:rank] = weighted_high
    left_out[:, rank : 2 * rank] = weighted_high
    left_out[:, 2 * rank : 3 * rank] = weighted_low

    half_copy.wait_send()
    fwd_copy.wait_send()
    loop(1, PLANE, lambda d: rs_copy(d).wait_send())
    loop(1, PLANE, lambda d: ag_copy(d).wait_send())
    loop(1, DEPTH, lambda d: z_copy(d).wait_send())

    def rows_wait_send(index):
        @pl.when(rows_target(index) != row)
        def _():
            rows_copy(index).wait_send()

    loop(0, DEPTH, rows_wait_send)
    for which in range(2):
        loop(1, PLANE, lambda d: a_copy(which, d).wait_send())
        loop(1, 2 * DEPTH, lambda d: b_copy(which, d).wait_send())
        loop(1, PLANE, lambda d: c_copy(which, d).wait_send())


def solve(covariance, estimate, dual_var, start_basis):
    rows, cols = covariance.shape
    rank = start_basis.shape[1]
    vmem = pl.BlockSpec(memory_space=pltpu.VMEM)
    hbm = pl.BlockSpec(memory_space=pl.ANY)
    dma = pltpu.SemaphoreType.DMA
    chunk = (CHUNK, rank)
    return pl.pallas_call(
        solve_kernel,
        out_shape=(
            jax.ShapeDtypeStruct((rows, 3 * rank), BF16),
            jax.ShapeDtypeStruct((cols, 3 * rank), BF16),
        ),
        in_specs=[hbm, hbm, hbm, vmem],
        out_specs=(vmem, vmem),
        scratch_shapes=[
            pltpu.VMEM((rows, cols), BF16),
            pltpu.VMEM((rows, cols), BF16),
            pltpu.VMEM((rows, cols), BF16),
            pltpu.VMEM((rows, cols), BF16),
            pltpu.VMEM((rows, cols), BF16),
            pltpu.VMEM((PLANE, *chunk), F32),
            pltpu.VMEM((PLANE, *chunk), F32),
            pltpu.VMEM((PLANE, *chunk), F32),
            pltpu.VMEM((PLANE, *chunk), F32),
            pltpu.VMEM((PLANE, *chunk), F32),
            pltpu.VMEM((2 * PLANE, *chunk), F32),
            pltpu.VMEM((DEPTH, *chunk), F32),
            pltpu.VMEM((8, *chunk), F32),
            pltpu.VMEM((rows, rank), F32),
            pltpu.VMEM((2, PLANE, 8, rank), F32),
            pltpu.VMEM((2, PLANE, 8, rank), F32),
            pltpu.VMEM((2, 8, rank), F32),
            pltpu.VMEM((2, 2 * DEPTH, 8, rank), F32),
            pltpu.VMEM((2, PLANE, 8, rank), F32),
            pltpu.VMEM((rank, 2 * rank), F32),
            pltpu.VMEM((2 * rank, rank), F32),
            dma((3, 2)),
            dma,
            dma,
            dma((PLANE,)),
            dma((PLANE,)),
            dma((PLANE,)),
            dma((PLANE,)),
            dma,
            dma,
            dma((DEPTH,)),
            dma((DEPTH,)),
            dma((8,)),
            dma((8,)),
            dma((2, PLANE)),
            dma((2, PLANE)),
            dma((2, 2 * DEPTH)),
            dma((2, 2 * DEPTH)),
            dma((2, PLANE)),
            dma((2, PLANE)),
        ],
        compiler_params=pltpu.CompilerParams(
            collective_id=0, has_side_effects=True, vmem_limit_bytes=48 * 1024 * 1024
        ),
        name="solve",
    )(covariance, estimate, dual_var, start_basis)


def finish_kernel(left, right, dual, estimate_out, dual_out):
    width = dual.shape[1]
    theta = dot(left[...], right[...], NT)
    row_start = lax.axis_index("row") * theta.shape[0]
    col_start = lax.axis_index("col") * (width * pl.num_programs(0)) + pl.program_id(0) * width
    row_ids = lax.broadcasted_iota(jnp.int32, theta.shape, 0)
    col_ids = lax.broadcasted_iota(jnp.int32, theta.shape, 1)
    theta = theta + jnp.where(row_ids + (row_start - col_start) == col_ids, base_level, 0.0)
    mixture = theta + dual[...].astype(F32)
    clipped = jnp.clip(mixture, -threshold, threshold)
    estimate_out[...] = mixture - clipped
    dual_out[...] = clipped.astype(BF16)


def finish(left, right, dual_var):
    rows, cols = dual_var.shape
    width = 256
    depth = left.shape[1]
    tile = pl.BlockSpec((rows, width), lambda n: (0, n))
    return pl.pallas_call(
        finish_kernel,
        grid=(cols // width,),
        out_shape=(
            jax.ShapeDtypeStruct((rows, cols), F32),
            jax.ShapeDtypeStruct((rows, cols), BF16),
        ),
        in_specs=[
            pl.BlockSpec((rows, depth), lambda n: (0, 0)),
            pl.BlockSpec((width, depth), lambda n: (n, 0)),
            tile,
        ],
        out_specs=(tile, tile),
        name="finish",
    )(left, right, dual_var)


def body(covariance, estimate, dual_var, start_basis):
    left, right = solve(covariance, estimate, dual_var, start_basis)
    return finish(left, right, dual_var)


def solution(mesh):
    return jax.shard_map(
        body,
        mesh=mesh,
        in_specs=(P("row", "col"), P("row", "col"), P("row", "col"), P("row", None)),
        out_specs=(P("row", "col"), P("row", "col")),
        check_vma=False,
    )
```

```python
import functools

import jax
import jax.numpy as jnp
from jax import lax
from jax.experimental import pallas as pl
from jax.experimental.pallas import tpu as pltpu
from jax.sharding import PartitionSpec as P

NS_ITERS = 12
MESH = pl.DeviceIdType.MESH
F32 = jnp.float32
BF16 = jnp.bfloat16

penalty = 0.01
threshold = 0.2
base_level = 10.0
highest = lax.Precision.HIGHEST

NN = (((1,), (0,)), ((), ()))
NT = (((1,), (1,)), ((), ()))
TN = (((0,), (0,)), ((), ()))

PLANE = 16
DEPTH = 8
CHUNK = 64
SOLVE_VMEM = 50500 * 1024
FINISH_VMEM = 32 * 1024 * 1024


def dot(left, right, dims=NN):
    return lax.dot_general(left, right, dims, preferred_element_type=F32)


def dot_full(left, right, dims=NN):
    return lax.dot_general(left, right, dims, precision=highest, preferred_element_type=F32)


def split(array):
    high = array.astype(BF16)
    return high, (array - high.astype(F32)).astype(BF16)


def dot_split(left, right, dims=NN):
    left_high, left_low = split(left)
    right_high, right_low = split(right)
    return dot(left_high, right_high, dims) + (
        dot(left_low, right_high, dims) + dot(left_high, right_low, dims)
    )


def loop(low, high, body):
    def step(index, carry):
        body(index)
        return carry

    lax.fori_loop(low, high, step, 0)


def arrived(ref, sem):
    pltpu.make_async_copy(ref, ref, sem).wait()


class Phase:
    def __init__(self):
        self.scope = None

    def __call__(self, name):
        if self.scope is not None:
            self.scope.__exit__(None, None, None)
        self.scope = None
        if name is not None:
            self.scope = jax.named_scope(name)
            self.scope.__enter__()


def solve_kernel(
    cov_hbm,
    est_hbm,
    dual_hbm,
    basis_hbm,
    left_out,
    right_out,
    dual,
    cov,
    est,
    basis,
    a_high,
    a_low,
    part_other,
    part_own,
    half_in,
    rs_send,
    rs_in,
    image,
    z_in,
    rows_in,
    product,
    red_part,
    red_in,
    red_mid,
    red_mid_in,
    red_out,
    table,
    load_sem,
    basis_sem,
    half_send,
    half_recv,
    rs_ssem,
    rs_rsem,
    ag_ssem,
    ag_rsem,
    fwd_send,
    fwd_recv,
    z_ssem,
    z_rsem,
    rows_ssem,
    rows_rsem,
    a_ssem,
    a_rsem,
    b_ssem,
    b_rsem,
    c_ssem,
    c_rsem,
):
    phase = Phase()
    phase("signal")
    row = lax.axis_index("row")
    col = lax.axis_index("col")
    core = lax.rem(row, 2)
    chip = lax.div(row, 2)
    other = row + 1 - 2 * core
    own_chunk = core * PLANE + chip
    own_line = lax.div(chip, 4)

    rank = basis.shape[1]
    width = 4 * CHUNK
    half = a_high.shape[1] // 2
    order = tuple(lax.rem(own_line + turn, 4) for turn in (2, 1, 3, 0))

    def window_of(side, block):
        offset = (1 - core if side == 0 else core) * half
        return pl.ds(pl.multiple_of(offset + block * width, width), width)

    def load(index, side, turn):
        source, target = ((cov_hbm, cov), (est_hbm, est), (dual_hbm, dual))[index]
        window = window_of(side, order[turn])
        return pltpu.make_async_copy(
            source.at[:, window], target.at[:, window], load_sem.at[index, side, turn]
        )

    basis_load = pltpu.make_async_copy(basis_hbm, basis, basis_sem)
    basis_load.start()
    for turn in range(4):
        for side in range(2):
            for index in range(3):
                load(index, side, turn).start()

    def plane_row(offset):
        return 2 * lax.rem(chip + offset, PLANE) + core

    def column_device(offset):
        target = lax.rem(2 * col + core + offset, 2 * DEPTH)
        return (2 * chip + lax.rem(target, 2), lax.div(target, 2))

    def rows_source(index):
        chunk = 8 * lax.rem(row, 4) + index
        return 2 * lax.rem(chunk, PLANE) + lax.div(chunk, PLANE)

    def rows_target(index):
        return 4 * index + lax.div(own_chunk, 8)

    barrier = pltpu.get_barrier_semaphore()

    def signal(device):
        pl.semaphore_signal(barrier, inc=1, device_id=device, device_id_type=MESH)

    loop(1, PLANE, lambda d: signal((plane_row(d), col)))
    loop(1, 2 * DEPTH, lambda d: signal(column_device(d)))

    def signal_source(index):
        source = rows_source(index)

        @pl.when(source != row)
        def _():
            signal((source, col))

    loop(0, 8, signal_source)

    has_own = lax.rem(row, 4) == lax.div(own_chunk, 8)
    peers = PLANE - 1 + 2 * DEPTH - 1 + 8 - jnp.where(has_own, 1, 0)

    phase("first")
    basis_load.wait()
    flipped = basis[...].T
    flip_high, flip_low = split(flipped)
    flip_both = jnp.concatenate([flip_high, flip_low], axis=0)

    def partial_terms(side, turn, target):
        for index in range(3):
            load(index, side, turn).wait()
        window = window_of(side, order[turn])
        shifted = penalty * (
            est[:, window].astype(F32) - dual[:, window].astype(F32)
        ) - cov[:, window].astype(F32)
        high, low = split(shifted)
        a_high[:, window] = high
        a_low[:, window] = low
        both = dot(flip_both, high)
        terms = both[:rank] + both[rank:] + dot(flip_high, low)
        target[pl.ds(4 * order[turn], 4)] = terms.T.reshape(4, CHUNK, rank)

    def half_copy(turn):
        block = pl.ds(4 * order[turn], 4)
        return pltpu.make_async_remote_copy(
            src_ref=part_other.at[block],
            dst_ref=half_in.at[block],
            send_sem=half_send.at[turn],
            recv_sem=half_recv.at[turn],
            device_id=(other, col),
            device_id_type=MESH,
        )

    def rs_copy(target):
        return pltpu.make_async_remote_copy(
            src_ref=rs_send.at[target],
            dst_ref=rs_in.at[chip],
            send_sem=rs_ssem,
            recv_sem=rs_rsem,
            device_id=(2 * target + core, col),
            device_id_type=MESH,
        )

    def combine(turn):
        half_copy(turn).wait_recv()
        block = pl.ds(4 * order[turn], 4)
        rs_send[block] = part_own[block] + half_in[block]

        def send(index):
            target = 4 * order[turn] + index

            @pl.when(target != chip)
            def _():
                rs_copy(target).start()

        loop(0, 4, send)

    for turn in range(4):
        partial_terms(0, turn, part_other)
        if turn == 0:
            phase("barrier")
            pl.semaphore_wait(barrier, peers)
            phase("second")
        half_copy(turn).start()
        partial_terms(1, turn, part_own)
        if turn > 0:
            combine(turn - 1)
    combine(3)
    rs_in[chip] = rs_send[chip]
    phase("rs_wait")
    arrived(rs_in.at[pl.ds(0, PLANE - 1)], rs_rsem)
    phase("spread")
    total = rs_in[0]
    for d in range(1, PLANE):
        total = total + rs_in[d]
    image[own_chunk] = total
    z_in[col] = total

    def z_copy(d):
        return pltpu.make_async_remote_copy(
            src_ref=image.at[own_chunk],
            dst_ref=z_in.at[col],
            send_sem=z_ssem,
            recv_sem=z_rsem,
            device_id=(row, lax.rem(col + d, DEPTH)),
            device_id_type=MESH,
        )

    def ag_copy(d):
        return pltpu.make_async_remote_copy(
            src_ref=image.at[own_chunk],
            dst_ref=image.at[own_chunk],
            send_sem=ag_ssem,
            recv_sem=ag_rsem,
            device_id=(plane_row(d), col),
            device_id_type=MESH,
        )

    def a_copy(which, d):
        return pltpu.make_async_remote_copy(
            src_ref=red_part.at[which, lax.rem(chip + d, PLANE)],
            dst_ref=red_in.at[which, chip],
            send_sem=a_ssem.at[which],
            recv_sem=a_rsem.at[which],
            device_id=(plane_row(d), col),
            device_id_type=MESH,
        )

    def b_copy(which, d):
        return pltpu.make_async_remote_copy(
            src_ref=red_mid.at[which],
            dst_ref=red_mid_in.at[which, 2 * col + core],
            send_sem=b_ssem.at[which],
            recv_sem=b_rsem.at[which],
            device_id=column_device(d),
            device_id_type=MESH,
        )

    def c_copy(which, d):
        return pltpu.make_async_remote_copy(
            src_ref=red_out.at[which, chip],
            dst_ref=red_out.at[which, chip],
            send_sem=c_ssem.at[which],
            recv_sem=c_rsem.at[which],
            device_id=(plane_row(d), col),
            device_id_type=MESH,
        )

    def reduce_start(which, value):
        red_part[which] = value.reshape(PLANE, 8, rank)
        loop(1, PLANE, lambda d: a_copy(which, d).start())
        red_in[which, chip] = red_part[which, chip]

    def reduce_middle(which):
        arrived(red_in.at[which, pl.ds(0, PLANE - 1)], a_rsem.at[which])
        piece = red_in[which, 0]
        for d in range(1, PLANE):
            piece = piece + red_in[which, d]
        red_mid[which] = piece
        red_mid_in[which, 2 * col + core] = piece
        loop(1, 2 * DEPTH, lambda d: b_copy(which, d).start())

    def reduce_spread(which):
        arrived(red_mid_in.at[which, pl.ds(0, 2 * DEPTH - 1)], b_rsem.at[which])
        piece = red_mid_in[which, 0]
        for d in range(1, 2 * DEPTH):
            piece = piece + red_mid_in[which, d]
        red_out[which, chip] = piece
        loop(1, PLANE, lambda d: c_copy(which, d).start())

    def reduce_end(which):
        arrived(red_out.at[which, pl.ds(0, PLANE - 1)], c_rsem.at[which])
        return red_out[which].reshape(rank, rank)

    loop(1, DEPTH, lambda d: z_copy(d).start())
    reduce_start(0, dot_full(total, total, TN))
    loop(1, PLANE, lambda d: ag_copy(d).start())
    phase("g_mid")
    reduce_middle(0)

    phase("z_wait")
    arrived(z_in.at[pl.ds(0, DEPTH - 1)], z_rsem)
    phase("rows_send")
    slot = lax.rem(own_chunk, 8)

    def rows_copy(index):
        return pltpu.make_async_remote_copy(
            src_ref=z_in.at[index],
            dst_ref=rows_in.at[slot],
            send_sem=rows_ssem.at[index],
            recv_sem=rows_rsem.at[slot],
            device_id=(rows_target(index), col),
            device_id_type=MESH,
        )

    def rows_start(index):
        @pl.when(rows_target(index) != row)
        def _():
            rows_copy(index).start()

        @pl.when(rows_target(index) == row)
        def _():
            rows_in[slot] = z_in[index]

    loop(0, DEPTH, rows_start)

    phase("ag_wait")
    arrived(image.at[pl.ds(0, PLANE - 1)], ag_rsem)
    phase("product1")
    own_half = image.at[pl.ds(core * PLANE, PLANE)]
    fwd_copy = pltpu.make_async_remote_copy(
        src_ref=own_half,
        dst_ref=own_half,
        send_sem=fwd_send,
        recv_sem=fwd_recv,
        device_id=(other, col),
        device_id_type=MESH,
    )
    fwd_copy.start()

    def product_terms(side):
        which = core if side == 0 else 1 - core

        def split_block(index):
            values = image[pl.ds(which * PLANE + 4 * index, 4)].reshape(width, rank)
            high, low = split(values)
            window = pl.ds(pl.multiple_of(which * half + width * index, width), width)
            right_out[window, 0:rank] = high
            right_out[window, rank : 2 * rank] = low
            right_out[window, 2 * rank : 3 * rank] = high

        loop(0, half // width, split_block)
        inner = pl.ds(pl.multiple_of(which * half, half), half)

        def product_block(index):
            window = pl.ds(pl.multiple_of(256 * index, 256), 256)
            both = dot(a_high[window, inner], right_out[inner, 0 : 2 * rank])
            terms = both[:, :rank] + (
                both[:, rank:] + dot(a_low[window, inner], right_out[inner, 0:rank])
            )
            product[window, :] = terms if side == 0 else product[window, :] + terms

        loop(0, product.shape[0] // 256, product_block)

    product_terms(0)
    phase("fwd_wait")
    fwd_copy.wait_recv()
    phase("product2")
    product_terms(1)
    phase("g_spread")
    reduce_spread(0)

    def rows_wait(index):
        @pl.when(rows_source(index) != row)
        def _():
            pltpu.make_async_remote_copy(
                src_ref=z_in.at[index],
                dst_ref=rows_in.at[index],
                send_sem=rows_ssem.at[index],
                recv_sem=rows_rsem.at[index],
                device_id=(rows_source(index), col),
                device_id_type=MESH,
            ).wait_recv()

    phase("rows_wait")
    loop(0, 8, rows_wait)
    phase("h_part")
    row_image = rows_in[...].reshape(8 * CHUNK, rank)
    reduce_start(1, dot_split(row_image, product[...], TN))

    phase("g_end")
    row_ids = lax.broadcasted_iota(jnp.int32, (rank, rank), 0)
    col_ids = lax.broadcasted_iota(jnp.int32, (rank, rank), 1)
    identity = jnp.where(row_ids == col_ids, 1.0, 0.0).astype(F32)
    gram = reduce_end(0)
    table[:, :rank] = gram
    table[:, rank:] = identity
    group = 4

    def lane_of(values, lane):
        return jnp.sum(
            jnp.where(col_ids[: values.shape[0]] == lane, values, 0.0), axis=1, keepdims=True
        )

    def eliminate(step):
        first = step * group
        pivot_rows = [table[pl.ds(first + p, 1), :] for p in range(group)]
        left_part = table[:, :rank]
        columns = [lane_of(left_part, first + p) for p in range(group)]
        entry = {
            (p, q): lane_of(pivot_rows[p][:, :rank], first + q)
            for p in range(group)
            for q in range(p, group)
        }
        change = None
        for p in range(group):
            scale = 1.0 / entry[p, p]
            factor = jnp.where(row_ids[:, :1] > first + p, columns[p] * scale, 0.0)
            for q in range(p + 1, group):
                columns[q] = columns[q] - factor * entry[p, q]
                weight = entry[p, q] * scale
                pivot_rows[q] = pivot_rows[q] - weight * pivot_rows[p]
                for t in range(q, group):
                    entry[q, t] = entry[q, t] - weight * entry[p, t]
            term = factor * pivot_rows[p]
            change = term if change is None else change + term
        table[...] = table[...] - change

    phase("elim1")
    loop(0, 6, eliminate)
    phase("h_mid")
    reduce_middle(1)
    phase("elim2")
    loop(6, 22, eliminate)
    phase("h_spread")
    reduce_spread(1)
    phase("elim3")
    loop(22, rank // group, eliminate)
    pivots = jnp.sum(table[:, :rank] * identity, axis=1, keepdims=True)
    inverse = table[:, rank:] / jnp.sqrt(pivots)
    row_basis = dot_split(row_image, inverse, NT)

    phase("drain")
    for turn in range(4):
        half_copy(turn).wait_send()
    fwd_copy.wait_send()
    arrived(rs_send.at[pl.ds(0, PLANE - 1)], rs_ssem)
    arrived(image.at[pl.ds(0, PLANE - 1)], ag_ssem)
    arrived(z_in.at[pl.ds(0, DEPTH - 1)], z_ssem)

    def rows_wait_send(index):
        @pl.when(rows_target(index) != row)
        def _():
            rows_copy(index).wait_send()

    loop(0, DEPTH, rows_wait_send)

    phase("h_end")
    inner = reduce_end(1)
    phase("ritz")
    raw_ritz = dot_split(dot_split(inverse, inner), inverse, NT)
    ritz = 0.5 * (raw_ritz + raw_ritz.T)
    square = dot_split(ritz, ritz) + 4.0 * penalty * identity
    frobenius = jnp.sqrt(jnp.sum(square * square, keepdims=True))

    phase("newton")
    iterate = square / frobenius
    both = iterate
    for _ in range(NS_ITERS):
        factor = 0.5 * (3.0 * identity - both)
        factor_high, factor_low = split(factor)
        factor_both = jnp.concatenate([factor_high, factor_low], axis=1)

        def scaled(left, factor_both=factor_both, factor_high=factor_high):
            high, low = split(left)
            terms = dot(high, factor_both)
            return terms[:, :rank] + (terms[:, rank:] + dot(low, factor_high))

        both = scaled(scaled(both))
        iterate = scaled(iterate)
    phase("tail")
    response = (ritz + jnp.sqrt(frobenius) * iterate) / (2.0 * penalty) - base_level * identity
    weighted_high, weighted_low = split(dot_split(row_basis, dot_split(response, inverse)))
    left_out[:, 0:rank] = weighted_high
    left_out[:, rank : 2 * rank] = weighted_high
    left_out[:, 2 * rank : 3 * rank] = weighted_low
    for which in range(2):
        arrived(red_in.at[which, pl.ds(0, PLANE - 1)], a_ssem.at[which])
        arrived(red_mid_in.at[which, pl.ds(0, 2 * DEPTH - 1)], b_ssem.at[which])
        arrived(red_out.at[which, pl.ds(0, PLANE - 1)], c_ssem.at[which])
    phase(None)


def solve(covariance, estimate, dual_var, start_basis):
    rows, cols = covariance.shape
    rank = start_basis.shape[1]
    vmem = pl.BlockSpec(memory_space=pltpu.VMEM)
    hbm = pl.BlockSpec(memory_space=pltpu.HBM)
    dma = pltpu.SemaphoreType.DMA
    matrix = pltpu.VMEM((rows, cols), BF16)
    chunk = (CHUNK, rank)
    chunks = pltpu.VMEM((PLANE, *chunk), F32)
    pieces = pltpu.VMEM((2, PLANE, 8, rank), F32)
    return pl.pallas_call(
        solve_kernel,
        out_shape=(
            jax.ShapeDtypeStruct((rows, 3 * rank), BF16),
            jax.ShapeDtypeStruct((cols, 3 * rank), BF16),
            jax.ShapeDtypeStruct((rows, cols), BF16),
        ),
        in_specs=[hbm, hbm, hbm, hbm],
        out_specs=(vmem, vmem, vmem),
        scratch_shapes=[
            matrix,
            matrix,
            pltpu.VMEM((rows, rank), F32),
            matrix,
            matrix,
            chunks,
            chunks,
            chunks,
            chunks,
            chunks,
            pltpu.VMEM((2 * PLANE, *chunk), F32),
            pltpu.VMEM((DEPTH, *chunk), F32),
            pltpu.VMEM((8, *chunk), F32),
            pltpu.VMEM((rows, rank), F32),
            pieces,
            pieces,
            pltpu.VMEM((2, 8, rank), F32),
            pieces,
            pieces,
            pltpu.VMEM((rank, 2 * rank), F32),
            dma((3, 2, 4)),
            dma,
            dma((4,)),
            dma((4,)),
            dma,
            dma,
            dma,
            dma,
            dma,
            dma,
            dma,
            dma,
            dma((8,)),
            dma((8,)),
            dma((2,)),
            dma((2,)),
            dma((2,)),
            dma((2,)),
            dma((2,)),
            dma((2,)),
        ],
        compiler_params=pltpu.CompilerParams(
            collective_id=0, has_side_effects=True, vmem_limit_bytes=SOLVE_VMEM
        ),
        name="solve",
    )(covariance, estimate, dual_var, start_basis)


def finish_kernel(left, right, dual, estimate_hbm, dual_hbm, estimate_out, dual_out, out_sem):
    rows, cols = dual.shape
    width = rows
    row = lax.axis_index("row")
    on_diagonal = lax.div(row, cols // rows) == lax.axis_index("col")
    row_ids = lax.broadcasted_iota(jnp.int32, (rows, width), 0)
    col_ids = lax.broadcasted_iota(jnp.int32, (rows, width), 1)

    def copies(block):
        window = pl.ds(pl.multiple_of(block * width, width), width)
        return (
            pltpu.make_async_copy(
                estimate_out.at[:, window], estimate_hbm.at[:, window], out_sem.at[0, block]
            ),
            pltpu.make_async_copy(
                dual_out.at[:, window], dual_hbm.at[:, window], out_sem.at[1, block]
            ),
        )

    def tile(block):
        window = pl.ds(pl.multiple_of(block * width, width), width)
        theta = dot(left[...], right[pl.ds(pl.multiple_of(block * width, width), width), :], NT)
        level = jnp.where(
            on_diagonal & (block == lax.rem(row, cols // rows)), base_level, 0.0
        ).astype(F32)
        theta = theta + jnp.where(row_ids == col_ids, level, 0.0)
        mixture = theta + dual[:, window].astype(F32)
        clipped = jnp.clip(mixture, -threshold, threshold)
        estimate_out[:, window] = mixture - clipped
        dual_out[:, window] = clipped.astype(BF16)
        for copy in copies(block):
            copy.start()

    loop(0, cols // width, tile)
    for block in range(cols // width):
        for copy in copies(block):
            copy.wait()


def finish(left, right, dual_var):
    rows, cols = dual_var.shape
    vmem = pl.BlockSpec(memory_space=pltpu.VMEM)
    hbm = pl.BlockSpec(memory_space=pltpu.HBM)
    return pl.pallas_call(
        finish_kernel,
        out_shape=(
            jax.ShapeDtypeStruct((rows, cols), F32),
            jax.ShapeDtypeStruct((rows, cols), BF16),
        ),
        in_specs=[vmem, vmem, vmem],
        out_specs=(hbm, hbm),
        scratch_shapes=[
            pltpu.VMEM((rows, cols), F32),
            pltpu.VMEM((rows, cols), BF16),
            pltpu.SemaphoreType.DMA((2, cols // rows)),
        ],
        compiler_params=pltpu.CompilerParams(vmem_limit_bytes=FINISH_VMEM),
        name="finish",
    )(left, right, dual_var)


def body(covariance, estimate, dual_var, start_basis):
    left, right, dual_kept = solve(covariance, estimate, dual_var, start_basis)
    return finish(left, right, dual_kept)


def solution(mesh):
    return jax.shard_map(
        body,
        mesh=mesh,
        in_specs=(P("row", "col"), P("row", "col"), P("row", "col"), P("row", None)),
        out_specs=(P("row", "col"), P("row", "col")),
        check_vma=False,
    )
```

```python
import functools

import jax
import jax.numpy as jnp
from jax import lax
from jax.experimental import pallas as pl
from jax.experimental.pallas import tpu as pltpu
from jax.sharding import PartitionSpec as P

NS_ITERS = 12
MESH = pl.DeviceIdType.MESH
F32 = jnp.float32
BF16 = jnp.bfloat16

penalty = 0.01
threshold = 0.2
base_level = 10.0
highest = lax.Precision.HIGHEST

NN = (((1,), (0,)), ((), ()))
NT = (((1,), (1,)), ((), ()))
TN = (((0,), (0,)), ((), ()))

PLANE = 16
DEPTH = 8
CHUNK = 64
PARTS = 2
PART = CHUNK // PARTS


def ring(offset, size):
    return min(offset, size - offset)


PLANE_OFFSETS = sorted(
    ((dy, dx) for dy in range(4) for dx in range(4) if dy or dx),
    key=lambda o: -(ring(o[0], 4) + ring(o[1], 4)),
)
SHIFTS = (2, 1, 3, 0)
DEPTH_OFFSETS = sorted(range(1, DEPTH), key=lambda d: -ring(d, DEPTH))
COLUMN_OFFSETS = sorted(
    ((dz, dc) for dz in range(DEPTH) for dc in range(2) if dz or dc),
    key=lambda o: -(ring(o[0], DEPTH) + 0.5 * o[1]),
)
SOLVE_VMEM = 50500 * 1024
FINISH_VMEM = 32 * 1024 * 1024


def dot(left, right, dims=NN):
    return lax.dot_general(left, right, dims, preferred_element_type=F32)


def dot_full(left, right, dims=NN):
    return lax.dot_general(left, right, dims, precision=highest, preferred_element_type=F32)


def split(array):
    high = array.astype(BF16)
    return high, (array - high.astype(F32)).astype(BF16)


def dot_split(left, right, dims=NN):
    left_high, left_low = split(left)
    right_high, right_low = split(right)
    return dot(left_high, right_high, dims) + (
        dot(left_low, right_high, dims) + dot(left_high, right_low, dims)
    )


def loop(low, high, body):
    def step(index, carry):
        body(index)
        return carry

    lax.fori_loop(low, high, step, 0)


def arrived(ref, sem):
    pltpu.make_async_copy(ref, ref, sem).wait()


class Phase:
    def __init__(self):
        self.scope = None

    def __call__(self, name):
        if self.scope is not None:
            self.scope.__exit__(None, None, None)
        self.scope = None
        if name is not None:
            self.scope = jax.named_scope(name)
            self.scope.__enter__()


def solve_kernel(
    cov_hbm,
    est_hbm,
    dual_hbm,
    basis_hbm,
    left_out,
    right_out,
    dual,
    cov,
    est,
    basis,
    a_high,
    a_low,
    part_other,
    part_own,
    half_in,
    rs_send,
    rs_in,
    image,
    z_in,
    rows_in,
    product,
    red_part,
    red_in,
    red_mid,
    red_mid_in,
    red_out,
    table,
    load_sem,
    basis_sem,
    half_send,
    half_recv,
    rs_ssem,
    rs_rsem,
    ag_ssem,
    ag_rsem,
    fwd_send,
    fwd_recv,
    z_ssem,
    z_rsem,
    rows_ssem,
    rows_rsem,
    a_ssem,
    a_rsem,
    b_ssem,
    b_rsem,
    c_ssem,
    c_rsem,
):
    phase = Phase()
    phase("signal")
    row = lax.axis_index("row")
    col = lax.axis_index("col")
    core = lax.rem(row, 2)
    chip = lax.div(row, 2)
    other = row + 1 - 2 * core
    own_chunk = core * PLANE + chip
    own_line = lax.div(chip, 4)

    rank = basis.shape[1]
    width = 4 * CHUNK
    half = 4 * width

    def load(index, side, shift):
        source, target = ((cov_hbm, cov), (est_hbm, est), (dual_hbm, dual))[index]
        offset = (1 - core if side == 0 else core) * half + lax.rem(own_line + shift, 4) * width
        window = pl.ds(pl.multiple_of(offset, width), width)
        return pltpu.make_async_copy(
            source.at[:, window], target.at[4 * side + shift], load_sem.at[index, side, shift]
        )

    basis_load = pltpu.make_async_copy(basis_hbm, basis, basis_sem)
    basis_load.start()
    for shift in SHIFTS:
        for side in range(2):
            for index in range(3):
                load(index, side, shift).start()

    def plane_chip(offset):
        dy, dx = offset
        return 4 * lax.rem(own_line + dy, 4) + lax.rem(lax.rem(chip, 4) + dx, 4)

    plane_chips = [plane_chip(offset) for offset in PLANE_OFFSETS]

    def column_device(offset):
        dz, dc = offset
        return (2 * chip + lax.rem(core + dc, 2), lax.rem(col + dz, DEPTH))

    column_devices = [column_device(offset) for offset in COLUMN_OFFSETS]

    def rows_source(index):
        chunk = 8 * lax.rem(row, 4) + index
        return 2 * lax.rem(chunk, PLANE) + lax.div(chunk, PLANE)

    def rows_target(index):
        return 4 * index + lax.div(own_chunk, 8)

    barrier = pltpu.get_barrier_semaphore()

    def signal(device):
        pl.semaphore_signal(barrier, inc=1, device_id=device, device_id_type=MESH)

    for target in plane_chips:
        signal((2 * target + core, col))
    for device in column_devices:
        signal(device)

    def signal_source(index):
        source = rows_source(index)

        @pl.when(source != row)
        def _():
            signal((source, col))

    loop(0, 8, signal_source)

    has_own = lax.rem(row, 4) == lax.div(own_chunk, 8)
    peers = PLANE - 1 + 2 * DEPTH - 1 + 8 - jnp.where(has_own, 1, 0)

    phase("first")
    basis_load.wait()
    flipped = basis[...].T
    flip_high, flip_low = split(flipped)
    flip_both = jnp.concatenate([flip_high, flip_low], axis=0)

    def load_wait(shift):
        for side in range(2):
            for index in range(3):
                load(index, side, shift).wait()

    def partial_terms(shift):
        for side, target in ((0, part_other), (1, part_own)):
            slot = 4 * side + shift
            shifted = penalty * (est[slot].astype(F32) - dual[slot].astype(F32)) - cov[slot].astype(F32)
            high, low = split(shifted)
            a_high[slot] = high
            a_low[slot] = low
            both = dot(flip_both, high)
            terms = both[:rank] + (both[rank:] + dot(flip_high, low))
            target[4 * shift : 4 * shift + 4] = terms.T.reshape(4, CHUNK, rank)

    part_rows = [pl.ds(PART * part, PART) for part in range(PARTS)]

    def half_copy(shift):
        block = pl.ds(4 * shift, 4)
        return pltpu.make_async_remote_copy(
            src_ref=part_other.at[block],
            dst_ref=half_in.at[block],
            send_sem=half_send.at[shift],
            recv_sem=half_recv.at[shift],
            device_id=(other, col),
            device_id_type=MESH,
        )

    def rs_copy(part, place, target):
        return pltpu.make_async_remote_copy(
            src_ref=rs_send.at[place, part_rows[part]],
            dst_ref=rs_in.at[part, chip],
            send_sem=rs_ssem,
            recv_sem=rs_rsem.at[part],
            device_id=(2 * target + core, col),
            device_id_type=MESH,
        )

    def send_terms(part, shift):
        for turn in (2, 1, 3, 0):
            if shift or turn:
                place = 4 * shift + lax.rem(lax.rem(chip, 4) + turn, 4)
                target = 4 * lax.rem(own_line + shift, 4) + lax.rem(lax.rem(chip, 4) + turn, 4)
                rs_copy(part, place, target).start()

    def combine(shift):
        half_copy(shift).wait_recv()
        block = slice(4 * shift, 4 * shift + 4)
        rs_send[block] = part_own[block] + half_in[block]
        send_terms(0, shift)

    load_wait(SHIFTS[0])
    partial_terms(SHIFTS[0])
    phase("barrier")
    pl.semaphore_wait(barrier, peers)
    phase("second")
    half_copy(SHIFTS[0]).start()
    for shift in SHIFTS[1:]:
        load_wait(shift)
    for turn in range(1, 4):
        partial_terms(SHIFTS[turn])
        half_copy(SHIFTS[turn]).start()
        if turn > 1:
            combine(SHIFTS[turn - 2])
    phase("last")
    combine(SHIFTS[2])
    combine(SHIFTS[3])
    for part in range(1, PARTS):
        for shift in SHIFTS:
            send_terms(part, shift)
    own_place = lax.rem(chip, 4)
    def z_copy(part, d):
        return pltpu.make_async_remote_copy(
            src_ref=image.at[own_chunk, part_rows[part]],
            dst_ref=z_in.at[col, part_rows[part]],
            send_sem=z_ssem,
            recv_sem=z_rsem.at[part, d],
            device_id=(row, lax.rem(col + d, DEPTH)),
            device_id_type=MESH,
        )

    def ag_copy(part, target, lines):
        return pltpu.make_async_remote_copy(
            src_ref=image.at[own_chunk, part_rows[part]],
            dst_ref=image.at[own_chunk, part_rows[part]],
            send_sem=ag_ssem,
            recv_sem=ag_rsem.at[lines],
            device_id=(2 * target + core, col),
            device_id_type=MESH,
        )

    def a_copy(which, target):
        return pltpu.make_async_remote_copy(
            src_ref=red_part.at[which, target],
            dst_ref=red_in.at[which, chip],
            send_sem=a_ssem.at[which],
            recv_sem=a_rsem.at[which],
            device_id=(2 * target + core, col),
            device_id_type=MESH,
        )

    def b_copy(which, device):
        return pltpu.make_async_remote_copy(
            src_ref=red_mid.at[which],
            dst_ref=red_mid_in.at[which, 2 * col + core],
            send_sem=b_ssem.at[which],
            recv_sem=b_rsem.at[which],
            device_id=device,
            device_id_type=MESH,
        )

    def c_copy(which, target):
        return pltpu.make_async_remote_copy(
            src_ref=red_out.at[which, chip],
            dst_ref=red_out.at[which, chip],
            send_sem=c_ssem.at[which],
            recv_sem=c_rsem.at[which],
            device_id=(2 * target + core, col),
            device_id_type=MESH,
        )

    def reduce_start(which, value):
        red_part[which] = value.reshape(PLANE, 8, rank)
        for target in plane_chips:
            a_copy(which, target).start()
        red_in[which, chip] = red_part[which, chip]

    def reduce_middle(which):
        arrived(red_in.at[which, pl.ds(0, PLANE - 1)], a_rsem.at[which])
        piece = red_in[which, 0]
        for d in range(1, PLANE):
            piece = piece + red_in[which, d]
        red_mid[which] = piece
        red_mid_in[which, 2 * col + core] = piece
        for device in column_devices:
            b_copy(which, device).start()

    def reduce_spread(which):
        arrived(red_mid_in.at[which, pl.ds(0, 2 * DEPTH - 1)], b_rsem.at[which])
        piece = red_mid_in[which, 0]
        for d in range(1, 2 * DEPTH):
            piece = piece + red_mid_in[which, d]
        red_out[which, chip] = piece
        for target in plane_chips:
            c_copy(which, target).start()

    def reduce_end(which):
        arrived(red_out.at[which, pl.ds(0, PLANE - 1)], c_rsem.at[which])
        return red_out[which].reshape(rank, rank)

    for part in range(PARTS):
        phase(f"rs_wait{part}")
        arrived(rs_in.at[part, pl.ds(0, PLANE - 1)], rs_rsem.at[part])
        phase(f"spread{part}")
        rs_in[part, chip] = rs_send[own_place, part_rows[part]]
        terms = rs_in[part, 0]
        for d in range(1, PLANE):
            terms = terms + rs_in[part, d]
        image[own_chunk, part_rows[part]] = terms
        z_in[col, part_rows[part]] = terms
        for d in DEPTH_OFFSETS:
            z_copy(part, d).start()
        if part == PARTS - 1:
            total = image[own_chunk]
            reduce_start(0, dot_full(total, total, TN))
        for offset, target in zip(PLANE_OFFSETS, plane_chips, strict=True):
            ag_copy(part, target, offset[0]).start()

    slot = lax.rem(own_chunk, 8)

    def rows_copy(part, index):
        return pltpu.make_async_remote_copy(
            src_ref=z_in.at[index, part_rows[part]],
            dst_ref=rows_in.at[slot, part_rows[part]],
            send_sem=rows_ssem.at[part, index],
            recv_sem=rows_rsem.at[part, slot],
            device_id=(rows_target(index), col),
            device_id_type=MESH,
        )

    def rows_start(part, index):
        @pl.when(rows_target(index) != row)
        def _():
            rows_copy(part, index).start()

        @pl.when(rows_target(index) == row)
        def _():
            rows_in[slot, part_rows[part]] = z_in[index, part_rows[part]]

    def forward(part, d):
        arrived(z_in.at[0, part_rows[part]], z_rsem.at[part, d])
        rows_start(part, lax.rem(col + DEPTH - d, DEPTH))

    def fwd_copy(lines):
        line = lax.rem(own_line + 4 - lines, 4)
        chunks = image.at[pl.ds(core * PLANE + 4 * line, 4)]
        return pltpu.make_async_remote_copy(
            src_ref=chunks,
            dst_ref=chunks,
            send_sem=fwd_send.at[lines],
            recv_sem=fwd_recv.at[lines],
            device_id=(other, col),
            device_id_type=MESH,
        )

    def product_terms(side):
        which = core if side == 0 else 1 - core
        highs, lows = [], []
        for shift in range(4):
            block = which * PLANE + 4 * lax.rem(own_line + shift, 4)
            window = pl.ds(pl.multiple_of(block * CHUNK, width), width)
            high, low = split(image[pl.ds(block, 4)].reshape(width, rank))
            right_out[window, 0:rank] = high
            right_out[window, rank : 2 * rank] = low
            right_out[window, 2 * rank : 3 * rank] = high
            highs.append(high)
            lows.append(low)
        right_high = jnp.concatenate(highs, axis=0)
        right_both = jnp.concatenate([right_high, jnp.concatenate(lows, axis=0)], axis=1)
        slots = range(4 * (1 - side), 4 * (1 - side) + 4)
        for start in range(0, product.shape[0], 256):
            rows = pl.ds(start, 256)
            both = dot(jnp.concatenate([a_high[slot, rows] for slot in slots], axis=1), right_both)
            terms = both[:, :rank] + (
                both[:, rank:]
                + dot(jnp.concatenate([a_low[slot, rows] for slot in slots], axis=1), right_high)
            )
            product[rows] = product[rows] + terms if side else terms

    def line_in(lines):
        count = 4 if lines else 3
        arrived(image.at[pl.ds(0, count)], ag_rsem.at[lines])
        fwd_copy(lines).start()

    phase("z0")
    for part in range(PARTS):
        rows_start(part, col)
    for d in DEPTH_OFFSETS:
        forward(0, d)
    phase("g_mid")
    reduce_middle(0)
    phase("z1")
    for d in DEPTH_OFFSETS:
        forward(1, d)
    phase("lines")
    for lines in (2, 1, 3, 0):
        line_in(lines)
    phase("product0")
    product_terms(0)
    phase("fwd_wait")
    for lines in range(4):
        fwd_copy(lines).wait_recv()
    phase("product1")
    product_terms(1)

    def rows_wait(index):
        @pl.when(rows_source(index) != row)
        def _():
            for part in range(PARTS):
                arrived(rows_in.at[index, part_rows[part]], rows_rsem.at[part, index])

    phase("rows_wait")
    loop(0, 8, rows_wait)
    phase("h_part")
    row_image = rows_in[...].reshape(8 * CHUNK, rank)
    reduce_start(1, dot_split(row_image, product[...], TN))

    row_ids = lax.broadcasted_iota(jnp.int32, (rank, rank), 0)
    col_ids = lax.broadcasted_iota(jnp.int32, (rank, rank), 1)
    identity = jnp.where(row_ids == col_ids, 1.0, 0.0).astype(F32)
    group = 4

    def lane_of(values, lane):
        return jnp.sum(
            jnp.where(col_ids[: values.shape[0]] == lane, values, 0.0), axis=1, keepdims=True
        )

    def eliminate(step):
        first = step * group
        pivot_rows = [table[pl.ds(first + p, 1), :] for p in range(group)]
        left_part = table[:, :rank]
        columns = [lane_of(left_part, first + p) for p in range(group)]
        entry = {
            (p, q): lane_of(pivot_rows[p][:, :rank], first + q)
            for p in range(group)
            for q in range(p, group)
        }
        change = None
        for p in range(group):
            scale = 1.0 / entry[p, p]
            factor = jnp.where(row_ids[:, :1] > first + p, columns[p] * scale, 0.0)
            for q in range(p + 1, group):
                columns[q] = columns[q] - factor * entry[p, q]
                weight = entry[p, q] * scale
                pivot_rows[q] = pivot_rows[q] - weight * pivot_rows[p]
                for t in range(q, group):
                    entry[q, t] = entry[q, t] - weight * entry[p, t]
            term = factor * pivot_rows[p]
            change = term if change is None else change + term
        table[...] = table[...] - change

    phase("g_spread")
    reduce_spread(0)
    phase("h_mid")
    reduce_middle(1)
    phase("g_end")
    table[:, :rank] = reduce_end(0)
    table[:, rank:] = identity
    phase("elim1")
    loop(0, 14, eliminate)
    phase("h_spread")
    reduce_spread(1)
    phase("elim2")
    loop(14, rank // group, eliminate)
    pivots = jnp.sum(table[:, :rank] * identity, axis=1, keepdims=True)
    inverse = table[:, rank:] / jnp.sqrt(pivots)
    row_basis = dot_split(row_image, inverse, NT)

    phase("drain")
    for shift in range(4):
        half_copy(shift).wait_send()
    for lines in range(4):
        fwd_copy(lines).wait_send()
    arrived(rs_send.at[pl.ds(0, PLANE - 1)], rs_ssem)
    arrived(image.at[pl.ds(0, PLANE - 1)], ag_ssem)
    arrived(z_in.at[pl.ds(0, DEPTH - 1)], z_ssem)

    def rows_wait_send(index):
        @pl.when(rows_target(index) != row)
        def _():
            for part in range(PARTS):
                rows_copy(part, index).wait_send()

    loop(0, DEPTH, rows_wait_send)

    phase("h_end")
    inner = reduce_end(1)
    phase("ritz")
    raw_ritz = dot_split(dot_split(inverse, inner), inverse, NT)
    ritz = 0.5 * (raw_ritz + raw_ritz.T)
    square = dot_split(ritz, ritz) + 4.0 * penalty * identity
    frobenius = jnp.sqrt(jnp.sum(square * square, keepdims=True))

    phase("newton")
    iterate = square / frobenius
    both = iterate
    for _ in range(NS_ITERS):
        factor = 0.5 * (3.0 * identity - both)
        factor_high, factor_low = split(factor)
        factor_both = jnp.concatenate([factor_high, factor_low], axis=1)

        def scaled(left, factor_both=factor_both, factor_high=factor_high):
            high, low = split(left)
            terms = dot(high, factor_both)
            return terms[:, :rank] + (terms[:, rank:] + dot(low, factor_high))

        both = scaled(scaled(both))
        iterate = scaled(iterate)
    phase("tail")
    response = (ritz + jnp.sqrt(frobenius) * iterate) / (2.0 * penalty) - base_level * identity
    weighted_high, weighted_low = split(dot_split(row_basis, dot_split(response, inverse)))
    left_out[:, 0:rank] = weighted_high
    left_out[:, rank : 2 * rank] = weighted_high
    left_out[:, 2 * rank : 3 * rank] = weighted_low
    for which in range(2):
        arrived(red_in.at[which, pl.ds(0, PLANE - 1)], a_ssem.at[which])
        arrived(red_mid_in.at[which, pl.ds(0, 2 * DEPTH - 1)], b_ssem.at[which])
        arrived(red_out.at[which, pl.ds(0, PLANE - 1)], c_ssem.at[which])
    phase(None)


def solve(covariance, estimate, dual_var, start_basis):
    rows, cols = covariance.shape
    rank = start_basis.shape[1]
    vmem = pl.BlockSpec(memory_space=pltpu.VMEM)
    hbm = pl.BlockSpec(memory_space=pltpu.HBM)
    dma = pltpu.SemaphoreType.DMA
    matrix = pltpu.VMEM((8, rows, cols // 8), BF16)
    chunk = (CHUNK, rank)
    chunks = pltpu.VMEM((PLANE, *chunk), F32)
    pieces = pltpu.VMEM((2, PLANE, 8, rank), F32)
    return pl.pallas_call(
        solve_kernel,
        out_shape=(
            jax.ShapeDtypeStruct((rows, 3 * rank), BF16),
            jax.ShapeDtypeStruct((cols, 3 * rank), BF16),
            jax.ShapeDtypeStruct((8, rows, cols // 8), BF16),
        ),
        in_specs=[hbm, hbm, hbm, hbm],
        out_specs=(vmem, vmem, vmem),
        scratch_shapes=[
            matrix,
            matrix,
            pltpu.VMEM((rows, rank), F32),
            matrix,
            matrix,
            chunks,
            chunks,
            chunks,
            chunks,
            pltpu.VMEM((PARTS, PLANE, PART, rank), F32),
            pltpu.VMEM((2 * PLANE, *chunk), F32),
            pltpu.VMEM((DEPTH, *chunk), F32),
            pltpu.VMEM((8, *chunk), F32),
            pltpu.VMEM((rows, rank), F32),
            pieces,
            pieces,
            pltpu.VMEM((2, 8, rank), F32),
            pieces,
            pieces,
            pltpu.VMEM((rank, 2 * rank), F32),
            dma((3, 2, 4)),
            dma,
            dma((4,)),
            dma((4,)),
            dma,
            dma((PARTS,)),
            dma,
            dma((4,)),
            dma((4,)),
            dma((4,)),
            dma,
            dma((PARTS, DEPTH)),
            dma((PARTS, 8)),
            dma((PARTS, 8)),
            dma((2,)),
            dma((2,)),
            dma((2,)),
            dma((2,)),
            dma((2,)),
            dma((2,)),
        ],
        compiler_params=pltpu.CompilerParams(
            collective_id=0, has_side_effects=True, vmem_limit_bytes=SOLVE_VMEM
        ),
        name="solve",
    )(covariance, estimate, dual_var, start_basis)


def finish_kernel(left, right, dual, estimate_hbm, dual_hbm, estimate_out, dual_out, out_sem):
    rows, cols = estimate_out.shape
    width = rows
    row = lax.axis_index("row")
    own_line = lax.div(row, 8)
    on_diagonal = lax.div(row, cols // rows) == lax.axis_index("col")
    row_ids = lax.broadcasted_iota(jnp.int32, (rows, width), 0)
    col_ids = lax.broadcasted_iota(jnp.int32, (rows, width), 1)

    def copies(block):
        window = pl.ds(pl.multiple_of(block * width, width), width)
        return (
            pltpu.make_async_copy(
                estimate_out.at[:, window], estimate_hbm.at[:, window], out_sem.at[0, block]
            ),
            pltpu.make_async_copy(
                dual_out.at[:, window], dual_hbm.at[:, window], out_sem.at[1, block]
            ),
        )

    def dual_block(index):
        side = jnp.where(lax.div(index, 4) == lax.rem(row, 2), 1, 0)
        return dual[4 * side + lax.rem(index + 4 - own_line, 4)]

    def tile(block):
        window = pl.ds(pl.multiple_of(block * width, width), width)
        theta = dot(left[...], right[pl.ds(pl.multiple_of(block * width, width), width), :], NT)
        level = jnp.where(
            on_diagonal & (block == lax.rem(row, cols // rows)), base_level, 0.0
        ).astype(F32)
        theta = theta + jnp.where(row_ids == col_ids, level, 0.0)
        kept = jnp.concatenate([dual_block(2 * block), dual_block(2 * block + 1)], axis=1)
        mixture = theta + kept.astype(F32)
        clipped = jnp.clip(mixture, -threshold, threshold)
        estimate_out[:, window] = mixture - clipped
        dual_out[:, window] = clipped.astype(BF16)
        for copy in copies(block):
            copy.start()

    loop(0, cols // width, tile)
    for block in range(cols // width):
        for copy in copies(block):
            copy.wait()


def finish(left, right, dual_kept):
    rows, cols = left.shape[0], right.shape[0]
    vmem = pl.BlockSpec(memory_space=pltpu.VMEM)
    hbm = pl.BlockSpec(memory_space=pltpu.HBM)
    return pl.pallas_call(
        finish_kernel,
        out_shape=(
            jax.ShapeDtypeStruct((rows, cols), F32),
            jax.ShapeDtypeStruct((rows, cols), BF16),
        ),
        in_specs=[vmem, vmem, vmem],
        out_specs=(hbm, hbm),
        scratch_shapes=[
            pltpu.VMEM((rows, cols), F32),
            pltpu.VMEM((rows, cols), BF16),
            pltpu.SemaphoreType.DMA((2, cols // rows)),
        ],
        compiler_params=pltpu.CompilerParams(vmem_limit_bytes=FINISH_VMEM),
        name="finish",
    )(left, right, dual_kept)


def body(covariance, estimate, dual_var, start_basis):
    left, right, dual_kept = solve(covariance, estimate, dual_var, start_basis)
    return finish(left, right, dual_kept)


def solution(mesh):
    return jax.shard_map(
        body,
        mesh=mesh,
        in_specs=(P("row", "col"), P("row", "col"), P("row", "col"), P("row", None)),
        out_specs=(P("row", "col"), P("row", "col")),
        check_vma=False,
    )
```

```python
import functools

import jax
import jax.numpy as jnp
from jax import lax
from jax.experimental import pallas as pl
from jax.experimental.pallas import tpu as pltpu
from jax.sharding import PartitionSpec as P

NS_ITERS = 12
MESH = pl.DeviceIdType.MESH
F32 = jnp.float32
BF16 = jnp.bfloat16

penalty = 0.01
threshold = 0.2
base_level = 10.0
highest = lax.Precision.HIGHEST

NN = (((1,), (0,)), ((), ()))
NT = (((1,), (1,)), ((), ()))
TN = (((0,), (0,)), ((), ()))

PLANE = 16
DEPTH = 8
CHUNK = 64
PARTS = 2
PART = CHUNK // PARTS


def ring(offset, size):
    return min(offset, size - offset)


PLANE_OFFSETS = sorted(
    ((dy, dx) for dy in range(4) for dx in range(4) if dy or dx),
    key=lambda o: -(ring(o[0], 4) + ring(o[1], 4)),
)
SHIFTS = (2, 1, 3, 0)
DEPTH_OFFSETS = sorted(range(1, DEPTH), key=lambda d: -ring(d, DEPTH))
COLUMN_OFFSETS = sorted(
    ((dz, dc) for dz in range(DEPTH) for dc in range(2) if dz or dc),
    key=lambda o: -(ring(o[0], DEPTH) + 0.5 * o[1]),
)
SOLVE_VMEM = 50500 * 1024
FINISH_VMEM = 32 * 1024 * 1024


def dot(left, right, dims=NN):
    return lax.dot_general(left, right, dims, preferred_element_type=F32)


def dot_full(left, right, dims=NN):
    return lax.dot_general(left, right, dims, precision=highest, preferred_element_type=F32)


def split(array):
    high = array.astype(BF16)
    return high, (array - high.astype(F32)).astype(BF16)


def dot_split(left, right, dims=NN):
    left_high, left_low = split(left)
    right_high, right_low = split(right)
    return dot(left_high, right_high, dims) + (
        dot(left_low, right_high, dims) + dot(left_high, right_low, dims)
    )


def loop(low, high, body):
    def step(index, carry):
        body(index)
        return carry

    lax.fori_loop(low, high, step, 0)


def arrived(ref, sem):
    pltpu.make_async_copy(ref, ref, sem).wait()


class Phase:
    def __init__(self):
        self.scope = None

    def __call__(self, name):
        if self.scope is not None:
            self.scope.__exit__(None, None, None)
        self.scope = None
        if name is not None:
            self.scope = jax.named_scope(name)
            self.scope.__enter__()


def solve_kernel(
    cov_hbm,
    est_hbm,
    dual_hbm,
    basis_hbm,
    left_out,
    right_out,
    dual,
    cov,
    est,
    basis,
    a_high,
    a_low,
    part_other,
    part_own,
    half_in,
    rs_send,
    rs_in,
    image,
    z_in,
    rows_in,
    product,
    red_part,
    red_in,
    red_mid,
    red_mid_in,
    red_out,
    table,
    load_sem,
    basis_sem,
    half_send,
    half_recv,
    rs_ssem,
    rs_rsem,
    ag_ssem,
    ag_rsem,
    fwd_send,
    fwd_recv,
    z_ssem,
    z_rsem,
    rows_ssem,
    rows_rsem,
    red_ssem,
    a_rsem,
    b_rsem,
    c_rsem,
):
    phase = Phase()
    phase("signal")
    row = lax.axis_index("row")
    col = lax.axis_index("col")
    core = lax.rem(row, 2)
    chip = lax.div(row, 2)
    other = row + 1 - 2 * core
    own_chunk = core * PLANE + chip
    own_line = lax.div(chip, 4)

    rank = basis.shape[1]
    width = 4 * CHUNK
    half = 4 * width

    def load(index, side, shift):
        source, target = ((cov_hbm, cov), (est_hbm, est), (dual_hbm, dual))[index]
        offset = (1 - core if side == 0 else core) * half + lax.rem(own_line + shift, 4) * width
        window = pl.ds(pl.multiple_of(offset, width), width)
        return pltpu.make_async_copy(
            source.at[:, window], target.at[4 * side + shift], load_sem.at[shift]
        )

    basis_load = pltpu.make_async_copy(basis_hbm, basis, basis_sem)
    basis_load.start()
    for shift in SHIFTS[:1]:
        for side in range(2):
            for index in range(3):
                load(index, side, shift).start()

    def plane_chip(offset):
        dy, dx = offset
        return 4 * lax.rem(own_line + dy, 4) + lax.rem(lax.rem(chip, 4) + dx, 4)

    plane_chips = [plane_chip(offset) for offset in PLANE_OFFSETS]

    def column_device(offset):
        dz, dc = offset
        return (2 * chip + lax.rem(core + dc, 2), lax.rem(col + dz, DEPTH))

    column_devices = [column_device(offset) for offset in COLUMN_OFFSETS]

    def rows_source(index):
        chunk = 8 * lax.rem(row, 4) + index
        return 2 * lax.rem(chunk, PLANE) + lax.div(chunk, PLANE)

    def rows_target(index):
        return 4 * index + lax.div(own_chunk, 8)

    barrier = pltpu.get_barrier_semaphore()

    def signal(device):
        pl.semaphore_signal(barrier, inc=1, device_id=device, device_id_type=MESH)

    for target in plane_chips:
        signal((2 * target + core, col))
    for device in column_devices:
        signal(device)

    def signal_source(index):
        source = rows_source(index)

        @pl.when(source != row)
        def _():
            signal((source, col))

    loop(0, 8, signal_source)

    has_own = lax.rem(row, 4) == lax.div(own_chunk, 8)
    peers = PLANE - 1 + 2 * DEPTH - 1 + 8 - jnp.where(has_own, 1, 0)

    for shift in SHIFTS[1:]:
        for side in range(2):
            for index in range(3):
                load(index, side, shift).start()

    phase("first")
    basis_load.wait()
    flipped = basis[...].T
    flip_high, flip_low = split(flipped)
    flip_both = jnp.concatenate([flip_high, flip_low], axis=0)

    def load_wait(shift):
        arrived(a_high.at[pl.ds(0, 6)], load_sem.at[shift])

    def partial_terms(shift):
        for side, target in ((0, part_other), (1, part_own)):
            slot = 4 * side + shift
            shifted = penalty * (est[slot].astype(F32) - dual[slot].astype(F32)) - cov[slot].astype(F32)
            high, low = split(shifted)
            a_high[slot] = high
            a_low[slot] = low
            both = dot(flip_both, high)
            terms = both[:rank] + (both[rank:] + dot(flip_high, low))
            target[4 * shift : 4 * shift + 4] = terms.T.reshape(4, CHUNK, rank)

    part_rows = [pl.ds(PART * part, PART) for part in range(PARTS)]

    def half_copy(shift):
        block = pl.ds(4 * shift, 4)
        return pltpu.make_async_remote_copy(
            src_ref=part_other.at[block],
            dst_ref=half_in.at[block],
            send_sem=half_send,
            recv_sem=half_recv.at[shift],
            device_id=(other, col),
            device_id_type=MESH,
        )

    def rs_copy(part, place, target):
        return pltpu.make_async_remote_copy(
            src_ref=rs_send.at[place, part_rows[part]],
            dst_ref=rs_in.at[part, chip],
            send_sem=rs_ssem,
            recv_sem=rs_rsem.at[part],
            device_id=(2 * target + core, col),
            device_id_type=MESH,
        )

    def send_terms(part, shift):
        for turn in (2, 1, 3, 0):
            if shift or turn:
                place = 4 * shift + lax.rem(lax.rem(chip, 4) + turn, 4)
                target = 4 * lax.rem(own_line + shift, 4) + lax.rem(lax.rem(chip, 4) + turn, 4)
                rs_copy(part, place, target).start()

    def combine(shift):
        half_copy(shift).wait_recv()
        block = slice(4 * shift, 4 * shift + 4)
        rs_send[block] = part_own[block] + half_in[block]
        send_terms(0, shift)

    load_wait(SHIFTS[0])
    partial_terms(SHIFTS[0])
    phase("barrier")
    pl.semaphore_wait(barrier, peers)
    phase("second")
    half_copy(SHIFTS[0]).start()
    for shift in SHIFTS[1:]:
        load_wait(shift)
    for turn in range(1, 4):
        partial_terms(SHIFTS[turn])
        half_copy(SHIFTS[turn]).start()
        if turn > 1:
            combine(SHIFTS[turn - 2])
    phase("last")
    combine(SHIFTS[2])
    combine(SHIFTS[3])
    for part in range(1, PARTS):
        for shift in SHIFTS:
            send_terms(part, shift)
    own_place = lax.rem(chip, 4)
    def z_copy(part, d):
        return pltpu.make_async_remote_copy(
            src_ref=image.at[own_chunk, part_rows[part]],
            dst_ref=z_in.at[col, part_rows[part]],
            send_sem=z_ssem,
            recv_sem=z_rsem.at[part],
            device_id=(row, lax.rem(col + d, DEPTH)),
            device_id_type=MESH,
        )

    def ag_copy(part, target, lines):
        return pltpu.make_async_remote_copy(
            src_ref=image.at[own_chunk, part_rows[part]],
            dst_ref=image.at[own_chunk, part_rows[part]],
            send_sem=ag_ssem,
            recv_sem=ag_rsem.at[lines],
            device_id=(2 * target + core, col),
            device_id_type=MESH,
        )

    def a_copy(which, target):
        return pltpu.make_async_remote_copy(
            src_ref=red_part.at[which, target],
            dst_ref=red_in.at[which, chip],
            send_sem=red_ssem.at[which],
            recv_sem=a_rsem.at[which],
            device_id=(2 * target + core, col),
            device_id_type=MESH,
        )

    def b_copy(which, device):
        return pltpu.make_async_remote_copy(
            src_ref=red_mid.at[which],
            dst_ref=red_mid_in.at[which, 2 * col + core],
            send_sem=red_ssem.at[which],
            recv_sem=b_rsem.at[which],
            device_id=device,
            device_id_type=MESH,
        )

    def c_copy(which, target):
        return pltpu.make_async_remote_copy(
            src_ref=red_out.at[which, chip],
            dst_ref=red_out.at[which, chip],
            send_sem=red_ssem.at[which],
            recv_sem=c_rsem.at[which],
            device_id=(2 * target + core, col),
            device_id_type=MESH,
        )

    def reduce_start(which, value):
        red_part[which] = value.reshape(PLANE, 8, rank)
        for target in plane_chips:
            a_copy(which, target).start()
        red_in[which, chip] = red_part[which, chip]

    def reduce_middle(which):
        arrived(red_in.at[which, pl.ds(0, PLANE - 1)], a_rsem.at[which])
        piece = red_in[which, 0]
        for d in range(1, PLANE):
            piece = piece + red_in[which, d]
        red_mid[which] = piece
        red_mid_in[which, 2 * col + core] = piece
        for device in column_devices:
            b_copy(which, device).start()

    def reduce_spread(which):
        arrived(red_mid_in.at[which, pl.ds(0, 2 * DEPTH - 1)], b_rsem.at[which])
        piece = red_mid_in[which, 0]
        for d in range(1, 2 * DEPTH):
            piece = piece + red_mid_in[which, d]
        red_out[which, chip] = piece
        for target in plane_chips:
            c_copy(which, target).start()

    def reduce_end(which):
        arrived(red_out.at[which, pl.ds(0, PLANE - 1)], c_rsem.at[which])
        return red_out[which].reshape(rank, rank)

    for part in range(PARTS):
        phase(f"rs_wait{part}")
        arrived(rs_in.at[part, pl.ds(0, PLANE - 1)], rs_rsem.at[part])
        phase(f"spread{part}")
        rs_in[part, chip] = rs_send[own_place, part_rows[part]]
        terms = rs_in[part, 0]
        for d in range(1, PLANE):
            terms = terms + rs_in[part, d]
        image[own_chunk, part_rows[part]] = terms
        z_in[col, part_rows[part]] = terms
        for d in DEPTH_OFFSETS:
            z_copy(part, d).start()
        if part == PARTS - 1:
            total = image[own_chunk]
            reduce_start(0, dot_full(total, total, TN))
        for offset, target in zip(PLANE_OFFSETS, plane_chips, strict=True):
            ag_copy(part, target, offset[0]).start()

    slot = lax.rem(own_chunk, 8)
    part_bytes = rs_in.at[0]

    def rows_copy(part, index):
        return pltpu.make_async_remote_copy(
            src_ref=z_in.at[index, part_rows[part]],
            dst_ref=rows_in.at[slot, part_rows[part]],
            send_sem=rows_ssem,
            recv_sem=rows_rsem,
            device_id=(rows_target(index), col),
            device_id_type=MESH,
        )

    def rows_start(part, index):
        @pl.when(rows_target(index) != row)
        def _():
            rows_copy(part, index).start()

        @pl.when(rows_target(index) == row)
        def _():
            rows_in[slot, part_rows[part]] = z_in[index, part_rows[part]]

    def forward(part):
        arrived(part_bytes.at[pl.ds(0, DEPTH - 1)], z_rsem.at[part])
        for d in DEPTH_OFFSETS:
            rows_start(part, lax.rem(col + DEPTH - d, DEPTH))

    def fwd_copy(lines):
        line = lax.rem(own_line + 4 - lines, 4)
        chunks = image.at[pl.ds(core * PLANE + 4 * line, 4)]
        return pltpu.make_async_remote_copy(
            src_ref=chunks,
            dst_ref=chunks,
            send_sem=fwd_send,
            recv_sem=fwd_recv,
            device_id=(other, col),
            device_id_type=MESH,
        )

    def product_terms(side):
        which = core if side == 0 else 1 - core
        highs, lows = [], []
        for shift in range(4):
            block = which * PLANE + 4 * lax.rem(own_line + shift, 4)
            window = pl.ds(pl.multiple_of(block * CHUNK, width), width)
            high, low = split(image[pl.ds(block, 4)].reshape(width, rank))
            right_out[window, 0:rank] = high
            right_out[window, rank : 2 * rank] = low
            right_out[window, 2 * rank : 3 * rank] = high
            highs.append(high)
            lows.append(low)
        right_high = jnp.concatenate(highs, axis=0)
        right_both = jnp.concatenate([right_high, jnp.concatenate(lows, axis=0)], axis=1)
        slots = range(4 * (1 - side), 4 * (1 - side) + 4)
        for start in range(0, product.shape[0], 256):
            rows = pl.ds(start, 256)
            both = dot(jnp.concatenate([a_high[slot, rows] for slot in slots], axis=1), right_both)
            terms = both[:, :rank] + (
                both[:, rank:]
                + dot(jnp.concatenate([a_low[slot, rows] for slot in slots], axis=1), right_high)
            )
            product[rows] = product[rows] + terms if side else terms

    def line_in(lines):
        count = 4 if lines else 3
        arrived(image.at[pl.ds(0, count)], ag_rsem.at[lines])
        fwd_copy(lines).start()

    phase("z0")
    for part in range(PARTS):
        rows_start(part, col)
    for part in range(PARTS - 1):
        forward(part)
    phase("g_mid")
    reduce_middle(0)
    phase("z1")
    forward(PARTS - 1)
    phase("lines")
    for lines in (2, 1, 3, 0):
        line_in(lines)
    phase("product0")
    product_terms(0)
    phase("fwd_wait")
    arrived(part_other, fwd_recv)
    phase("product1")
    product_terms(1)

    def rows_done(sem):
        @pl.when(has_own)
        def _():
            arrived(rows_in.at[pl.ds(0, 7)], sem)

        @pl.when(jnp.logical_not(has_own))
        def _():
            arrived(rows_in, sem)

    phase("rows_wait")
    rows_done(rows_rsem)
    phase("h_part")
    row_image = rows_in[...].reshape(8 * CHUNK, rank)
    reduce_start(1, dot_split(row_image, product[...], TN))

    row_ids = lax.broadcasted_iota(jnp.int32, (rank, rank), 0)
    col_ids = lax.broadcasted_iota(jnp.int32, (rank, rank), 1)
    identity = jnp.where(row_ids == col_ids, 1.0, 0.0).astype(F32)
    group = 4

    def lane_of(values, lane):
        return jnp.sum(
            jnp.where(col_ids[: values.shape[0]] == lane, values, 0.0), axis=1, keepdims=True
        )

    def eliminate(step):
        first = step * group
        pivot_rows = [table[pl.ds(first + p, 1), :] for p in range(group)]
        left_part = table[:, :rank]
        columns = [lane_of(left_part, first + p) for p in range(group)]
        entry = {
            (p, q): lane_of(pivot_rows[p][:, :rank], first + q)
            for p in range(group)
            for q in range(p, group)
        }
        change = None
        for p in range(group):
            scale = 1.0 / entry[p, p]
            factor = jnp.where(row_ids[:, :1] > first + p, columns[p] * scale, 0.0)
            for q in range(p + 1, group):
                columns[q] = columns[q] - factor * entry[p, q]
                weight = entry[p, q] * scale
                pivot_rows[q] = pivot_rows[q] - weight * pivot_rows[p]
                for t in range(q, group):
                    entry[q, t] = entry[q, t] - weight * entry[p, t]
            term = factor * pivot_rows[p]
            change = term if change is None else change + term
        table[...] = table[...] - change

    phase("g_spread")
    reduce_spread(0)
    phase("h_mid")
    reduce_middle(1)
    phase("g_end")
    table[:, :rank] = reduce_end(0)
    table[:, rank:] = identity
    phase("elim1")
    loop(0, 14, eliminate)
    phase("h_spread")
    reduce_spread(1)
    phase("elim2")
    loop(14, rank // group, eliminate)
    pivots = jnp.sum(table[:, :rank] * identity, axis=1, keepdims=True)
    inverse = table[:, rank:] / jnp.sqrt(pivots)
    row_basis = dot_split(row_image, inverse, NT)

    phase("drain")
    arrived(part_other, half_send)
    arrived(part_other, fwd_send)
    arrived(rs_send.at[pl.ds(0, PLANE - 1)], rs_ssem)
    arrived(image.at[pl.ds(0, PLANE - 1)], ag_ssem)
    arrived(z_in.at[pl.ds(0, DEPTH - 1)], z_ssem)

    rows_done(rows_ssem)

    phase("h_end")
    inner = reduce_end(1)
    phase("ritz")
    raw_ritz = dot_split(dot_split(inverse, inner), inverse, NT)
    ritz = 0.5 * (raw_ritz + raw_ritz.T)
    square = dot_split(ritz, ritz) + 4.0 * penalty * identity
    frobenius = jnp.sqrt(jnp.sum(square * square, keepdims=True))

    phase("newton")
    iterate = square / frobenius
    both = iterate
    for _ in range(NS_ITERS):
        factor = 0.5 * (3.0 * identity - both)
        factor_high, factor_low = split(factor)
        factor_both = jnp.concatenate([factor_high, factor_low], axis=1)

        def scaled(left, factor_both=factor_both, factor_high=factor_high):
            high, low = split(left)
            terms = dot(high, factor_both)
            return terms[:, :rank] + (terms[:, rank:] + dot(low, factor_high))

        both = scaled(scaled(both))
        iterate = scaled(iterate)
    phase("tail")
    response = (ritz + jnp.sqrt(frobenius) * iterate) / (2.0 * penalty) - base_level * identity
    weighted_high, weighted_low = split(dot_split(row_basis, dot_split(response, inverse)))
    left_out[:, 0:rank] = weighted_high
    left_out[:, rank : 2 * rank] = weighted_high
    left_out[:, 2 * rank : 3 * rank] = weighted_low
    for which in range(2):
        pieces = 2 * (PLANE - 1) + 2 * DEPTH - 1
        arrived(product.at[pl.ds(0, 8 * pieces)], red_ssem.at[which])
    phase(None)


def solve(covariance, estimate, dual_var, start_basis):
    rows, cols = covariance.shape
    rank = start_basis.shape[1]
    vmem = pl.BlockSpec(memory_space=pltpu.VMEM)
    hbm = pl.BlockSpec(memory_space=pltpu.HBM)
    dma = pltpu.SemaphoreType.DMA
    matrix = pltpu.VMEM((8, rows, cols // 8), BF16)
    chunk = (CHUNK, rank)
    chunks = pltpu.VMEM((PLANE, *chunk), F32)
    pieces = pltpu.VMEM((2, PLANE, 8, rank), F32)
    return pl.pallas_call(
        solve_kernel,
        out_shape=(
            jax.ShapeDtypeStruct((rows, 3 * rank), BF16),
            jax.ShapeDtypeStruct((cols, 3 * rank), BF16),
            jax.ShapeDtypeStruct((8, rows, cols // 8), BF16),
        ),
        in_specs=[hbm, hbm, hbm, hbm],
        out_specs=(vmem, vmem, vmem),
        scratch_shapes=[
            matrix,
            matrix,
            pltpu.VMEM((rows, rank), F32),
            matrix,
            matrix,
            chunks,
            chunks,
            chunks,
            chunks,
            pltpu.VMEM((PARTS, PLANE, PART, rank), F32),
            pltpu.VMEM((2 * PLANE, *chunk), F32),
            pltpu.VMEM((DEPTH, *chunk), F32),
            pltpu.VMEM((8, *chunk), F32),
            pltpu.VMEM((rows, rank), F32),
            pieces,
            pieces,
            pltpu.VMEM((2, 8, rank), F32),
            pieces,
            pieces,
            pltpu.VMEM((rank, 2 * rank), F32),
            dma((4,)),
            dma,
            dma,
            dma((4,)),
            dma,
            dma((PARTS,)),
            dma,
            dma((4,)),
            dma,
            dma,
            dma,
            dma((PARTS,)),
            dma,
            dma,
            dma((2,)),
            dma((2,)),
            dma((2,)),
            dma((2,)),
        ],
        compiler_params=pltpu.CompilerParams(
            collective_id=0, has_side_effects=True, vmem_limit_bytes=SOLVE_VMEM
        ),
        name="solve",
    )(covariance, estimate, dual_var, start_basis)


def finish_kernel(left, right, dual, estimate_hbm, dual_hbm, estimate_out, dual_out, out_sem):
    rows, cols = estimate_out.shape
    width = rows
    row = lax.axis_index("row")
    own_line = lax.div(row, 8)
    on_diagonal = lax.div(row, cols // rows) == lax.axis_index("col")
    row_ids = lax.broadcasted_iota(jnp.int32, (rows, width), 0)
    col_ids = lax.broadcasted_iota(jnp.int32, (rows, width), 1)

    def copies(block):
        window = pl.ds(block * width, width)
        return (
            pltpu.make_async_copy(
                estimate_out.at[:, window], estimate_hbm.at[:, window], out_sem.at[0, block]
            ),
            pltpu.make_async_copy(
                dual_out.at[:, window], dual_hbm.at[:, window], out_sem.at[1, block]
            ),
        )

    def dual_block(index):
        side = jnp.where(index // 4 == lax.rem(row, 2), 1, 0)
        return dual[4 * side + lax.rem(index + 4 - own_line, 4)]

    def tile(block):
        window = pl.ds(block * width, width)
        theta = dot(left[...], right[window, :], NT)
        level = jnp.where(
            on_diagonal & (block == lax.rem(row, cols // rows)), base_level, 0.0
        ).astype(F32)
        theta = theta + jnp.where(row_ids == col_ids, level, 0.0)
        kept = jnp.concatenate([dual_block(2 * block), dual_block(2 * block + 1)], axis=1)
        mixture = theta + kept.astype(F32)
        clipped = jnp.clip(mixture, -threshold, threshold)
        estimate_out[:, window] = mixture - clipped
        dual_out[:, window] = clipped.astype(BF16)
        for copy in copies(block):
            copy.start()

    for block in range(cols // width):
        tile(block)
    for block in range(cols // width):
        for copy in copies(block):
            copy.wait()


def finish(left, right, dual_kept):
    rows, cols = left.shape[0], right.shape[0]
    vmem = pl.BlockSpec(memory_space=pltpu.VMEM)
    hbm = pl.BlockSpec(memory_space=pltpu.HBM)
    return pl.pallas_call(
        finish_kernel,
        out_shape=(
            jax.ShapeDtypeStruct((rows, cols), F32),
            jax.ShapeDtypeStruct((rows, cols), BF16),
        ),
        in_specs=[vmem, vmem, vmem],
        out_specs=(hbm, hbm),
        scratch_shapes=[
            pltpu.VMEM((rows, cols), F32),
            pltpu.VMEM((rows, cols), BF16),
            pltpu.SemaphoreType.DMA((2, cols // rows)),
        ],
        compiler_params=pltpu.CompilerParams(vmem_limit_bytes=FINISH_VMEM),
        name="finish",
    )(left, right, dual_kept)


def body(covariance, estimate, dual_var, start_basis):
    start_basis = pltpu.with_memory_space_constraint(start_basis, pltpu.HBM)
    left, right, dual_kept = solve(covariance, estimate, dual_var, start_basis)
    return finish(left, right, dual_kept)


def solution(mesh):
    return jax.shard_map(
        body,
        mesh=mesh,
        in_specs=(P("row", "col"), P("row", "col"), P("row", "col"), P("row", None)),
        out_specs=(P("row", "col"), P("row", "col")),
        check_vma=False,
    )
```

```python
import functools

import jax
import jax.numpy as jnp
from jax import lax
from jax.experimental import pallas as pl
from jax.experimental.pallas import tpu as pltpu
from jax.sharding import PartitionSpec as P

NS_ITERS = 12
MESH = pl.DeviceIdType.MESH
F32 = jnp.float32
BF16 = jnp.bfloat16

penalty = 0.01
threshold = 0.2
base_level = 10.0
highest = lax.Precision.HIGHEST

NN = (((1,), (0,)), ((), ()))
NT = (((1,), (1,)), ((), ()))
TN = (((0,), (0,)), ((), ()))

PLANE = 16
DEPTH = 8
CHUNK = 64
PARTS = 2
PART = CHUNK // PARTS


def ring(offset, size):
    return min(offset, size - offset)


PLANE_OFFSETS = sorted(
    ((dy, dx) for dy in range(4) for dx in range(4) if dy or dx),
    key=lambda o: -(ring(o[0], 4) + ring(o[1], 4)),
)
SHIFTS = (2, 1, 3, 0)
DEPTH_OFFSETS = sorted(range(1, DEPTH), key=lambda d: -ring(d, DEPTH))
COLUMN_OFFSETS = sorted(
    ((dz, dc) for dz in range(DEPTH) for dc in range(2) if dz or dc),
    key=lambda o: -(ring(o[0], DEPTH) + 0.5 * o[1]),
)
SOLVE_VMEM = 50500 * 1024
FINISH_VMEM = 32 * 1024 * 1024


def dot(left, right, dims=NN):
    return lax.dot_general(left, right, dims, preferred_element_type=F32)


def dot_full(left, right, dims=NN):
    return lax.dot_general(left, right, dims, precision=highest, preferred_element_type=F32)


def split(array):
    high = array.astype(BF16)
    return high, (array - high.astype(F32)).astype(BF16)


def dot_split(left, right, dims=NN):
    left_high, left_low = split(left)
    right_high, right_low = split(right)
    return dot(left_high, right_high, dims) + (
        dot(left_low, right_high, dims) + dot(left_high, right_low, dims)
    )


def loop(low, high, body):
    def step(index, carry):
        body(index)
        return carry

    lax.fori_loop(low, high, step, 0)


def arrived(ref, sem):
    pltpu.make_async_copy(ref, ref, sem).wait()


class Phase:
    def __init__(self):
        self.scope = None

    def __call__(self, name):
        if self.scope is not None:
            self.scope.__exit__(None, None, None)
        self.scope = None
        if name is not None:
            self.scope = jax.named_scope(name)
            self.scope.__enter__()


def solve_kernel(
    cov_hbm,
    est_hbm,
    dual_hbm,
    basis_hbm,
    left_out,
    right_out,
    dual,
    cov,
    est,
    basis,
    a_high,
    a_low,
    part_other,
    part_own,
    half_in,
    rs_send,
    rs_in,
    image,
    z_in,
    rows_in,
    product,
    red_part,
    red_in,
    red_mid,
    red_mid_in,
    red_out,
    table,
    load_sem,
    basis_sem,
    half_send,
    half_recv,
    rs_ssem,
    rs_rsem,
    ag_ssem,
    ag_rsem,
    fwd_send,
    fwd_recv,
    z_ssem,
    z_rsem,
    rows_ssem,
    rows_rsem,
    red_ssem,
    a_rsem,
    b_rsem,
    c_rsem,
):
    phase = Phase()
    phase("signal")
    row = lax.axis_index("row")
    col = lax.axis_index("col")
    core = lax.rem(row, 2)
    chip = lax.div(row, 2)
    other = row + 1 - 2 * core
    own_chunk = core * PLANE + chip
    own_line = lax.div(chip, 4)

    rank = basis.shape[1]
    width = 4 * CHUNK
    half = 4 * width

    def load(index, side, shift):
        source, target = ((cov_hbm, cov), (est_hbm, est), (dual_hbm, dual))[index]
        offset = (1 - core if side == 0 else core) * half + lax.rem(own_line + shift, 4) * width
        window = pl.ds(pl.multiple_of(offset, width), width)
        return pltpu.make_async_copy(
            source.at[:, window], target.at[4 * side + shift], load_sem.at[shift]
        )

    basis_load = pltpu.make_async_copy(basis_hbm, basis, basis_sem)
    basis_load.start()
    for shift in SHIFTS[:1]:
        for side in range(2):
            for index in range(3):
                load(index, side, shift).start()

    def plane_chip(offset):
        dy, dx = offset
        return 4 * lax.rem(own_line + dy, 4) + lax.rem(lax.rem(chip, 4) + dx, 4)

    plane_chips = [plane_chip(offset) for offset in PLANE_OFFSETS]

    def column_device(offset):
        dz, dc = offset
        return (2 * chip + lax.rem(core + dc, 2), lax.rem(col + dz, DEPTH))

    column_devices = [column_device(offset) for offset in COLUMN_OFFSETS]

    def rows_source(index):
        chunk = 8 * lax.rem(row, 4) + index
        return 2 * lax.rem(chunk, PLANE) + lax.div(chunk, PLANE)

    def rows_target(index):
        return 4 * index + lax.div(own_chunk, 8)

    barrier = pltpu.get_barrier_semaphore()

    def signal(device):
        pl.semaphore_signal(barrier, inc=1, device_id=device, device_id_type=MESH)

    for target in plane_chips:
        signal((2 * target + core, col))
    for device in column_devices:
        signal(device)

    def signal_source(index):
        source = rows_source(index)

        @pl.when(source != row)
        def _():
            signal((source, col))

    loop(0, 8, signal_source)

    has_own = lax.rem(row, 4) == lax.div(own_chunk, 8)
    peers = PLANE - 1 + 2 * DEPTH - 1 + 8 - jnp.where(has_own, 1, 0)

    for shift in SHIFTS[1:]:
        for side in range(2):
            for index in range(3):
                load(index, side, shift).start()

    phase("first")
    basis_load.wait()
    flipped = basis[...].T
    flip_high, flip_low = split(flipped)
    flip_both = jnp.concatenate([flip_high, flip_low], axis=0)

    def load_wait(shift):
        arrived(a_high.at[pl.ds(0, 6)], load_sem.at[shift])

    def partial_terms(shift):
        for side, target in ((0, part_other), (1, part_own)):
            slot = 4 * side + shift
            shifted = penalty * (est[slot].astype(F32) - dual[slot].astype(F32)) - cov[slot].astype(F32)
            high, low = split(shifted)
            a_high[slot] = high
            a_low[slot] = low
            both = dot(flip_both, high)
            terms = both[:rank] + (both[rank:] + dot(flip_high, low))
            target[shift] = terms.T.reshape(PARTS, 4, PART, rank)

    own_place = lax.rem(chip, 4)

    def half_copy(shift):
        return pltpu.make_async_remote_copy(
            src_ref=part_other.at[shift],
            dst_ref=half_in.at[shift],
            send_sem=half_send,
            recv_sem=half_recv.at[shift],
            device_id=(other, col),
            device_id_type=MESH,
        )

    def rs_copy(part, shift, place, target):
        return pltpu.make_async_remote_copy(
            src_ref=rs_send.at[shift, part, place],
            dst_ref=rs_in.at[part, chip],
            send_sem=rs_ssem,
            recv_sem=rs_rsem.at[part],
            device_id=(2 * target + core, col),
            device_id_type=MESH,
        )

    def send_terms(part, shift):
        for turn in (2, 1, 3, 0):
            if shift or turn:
                place = lax.rem(own_place + turn, 4)
                target = 4 * lax.rem(own_line + shift, 4) + place
                rs_copy(part, shift, place, target).start()

    def combine(shift):
        half_copy(shift).wait_recv()
        rs_send[shift] = part_own[shift] + half_in[shift]
        send_terms(0, shift)

    load_wait(SHIFTS[0])
    partial_terms(SHIFTS[0])
    phase("barrier")
    pl.semaphore_wait(barrier, peers)
    phase("second")
    half_copy(SHIFTS[0]).start()
    for shift in SHIFTS[1:]:
        load_wait(shift)
    for turn in range(1, 4):
        partial_terms(SHIFTS[turn])
        half_copy(SHIFTS[turn]).start()
        if turn > 1:
            combine(SHIFTS[turn - 2])
    phase("last")
    combine(SHIFTS[2])
    combine(SHIFTS[3])
    for part in range(1, PARTS):
        for shift in SHIFTS:
            send_terms(part, shift)
    def own_piece(part):
        return image.at[core, own_line, part, own_place]

    def z_copy(part, d):
        return pltpu.make_async_remote_copy(
            src_ref=own_piece(part),
            dst_ref=z_in.at[col, part],
            send_sem=z_ssem,
            recv_sem=z_rsem.at[part],
            device_id=(row, lax.rem(col + d, DEPTH)),
            device_id_type=MESH,
        )

    def ag_copy(part, target, lines):
        return pltpu.make_async_remote_copy(
            src_ref=own_piece(part),
            dst_ref=own_piece(part),
            send_sem=ag_ssem,
            recv_sem=ag_rsem.at[part, lines],
            device_id=(2 * target + core, col),
            device_id_type=MESH,
        )

    def a_copy(which, target):
        return pltpu.make_async_remote_copy(
            src_ref=red_part.at[which, target],
            dst_ref=red_in.at[which, chip],
            send_sem=red_ssem.at[which],
            recv_sem=a_rsem.at[which],
            device_id=(2 * target + core, col),
            device_id_type=MESH,
        )

    def b_copy(which, device):
        return pltpu.make_async_remote_copy(
            src_ref=red_mid.at[which],
            dst_ref=red_mid_in.at[which, 2 * col + core],
            send_sem=red_ssem.at[which],
            recv_sem=b_rsem.at[which],
            device_id=device,
            device_id_type=MESH,
        )

    def c_copy(which, target):
        return pltpu.make_async_remote_copy(
            src_ref=red_out.at[which, chip],
            dst_ref=red_out.at[which, chip],
            send_sem=red_ssem.at[which],
            recv_sem=c_rsem.at[which],
            device_id=(2 * target + core, col),
            device_id_type=MESH,
        )

    def reduce_start(which, value):
        red_part[which] = value.reshape(PLANE, 8, rank)
        for target in plane_chips:
            a_copy(which, target).start()
        red_in[which, chip] = red_part[which, chip]

    def reduce_middle(which):
        arrived(red_in.at[which, pl.ds(0, PLANE - 1)], a_rsem.at[which])
        piece = red_in[which, 0]
        for d in range(1, PLANE):
            piece = piece + red_in[which, d]
        red_mid[which] = piece
        red_mid_in[which, 2 * col + core] = piece
        for device in column_devices:
            b_copy(which, device).start()

    def reduce_spread(which):
        arrived(red_mid_in.at[which, pl.ds(0, 2 * DEPTH - 1)], b_rsem.at[which])
        piece = red_mid_in[which, 0]
        for d in range(1, 2 * DEPTH):
            piece = piece + red_mid_in[which, d]
        red_out[which, chip] = piece
        for target in plane_chips:
            c_copy(which, target).start()

    def reduce_end(which):
        arrived(red_out.at[which, pl.ds(0, PLANE - 1)], c_rsem.at[which])
        return red_out[which].reshape(rank, rank)

    sums = []
    for part in range(PARTS):
        phase(f"rs_wait{part}")
        arrived(rs_in.at[part, pl.ds(0, PLANE - 1)], rs_rsem.at[part])
        phase(f"spread{part}")
        rs_in[part, chip] = rs_send[0, part, own_place]
        terms = rs_in[part, 0]
        for d in range(1, PLANE):
            terms = terms + rs_in[part, d]
        image[core, own_line, part, own_place] = terms
        z_in[col, part] = terms
        sums.append(terms)
        for d in DEPTH_OFFSETS:
            z_copy(part, d).start()
        gathers = [
            ag_copy(part, target, offset[0])
            for offset, target in zip(PLANE_OFFSETS, plane_chips, strict=True)
        ]
        first = 4 if part == PARTS - 1 else PLANE
        for copy in gathers[:first]:
            copy.start()
        if part == PARTS - 1:
            total = jnp.concatenate(sums, axis=0)
            reduce_start(0, dot_full(total, total, TN))
        for copy in gathers[first:]:
            copy.start()

    part_bytes = rs_in.at[0]

    def rows_copy(part, index):
        return pltpu.make_async_remote_copy(
            src_ref=z_in.at[index, part],
            dst_ref=rows_in.at[lax.rem(own_line, 2), part, own_place],
            send_sem=rows_ssem,
            recv_sem=rows_rsem,
            device_id=(rows_target(index), col),
            device_id_type=MESH,
        )

    def rows_start(part, index):
        @pl.when(rows_target(index) != row)
        def _():
            rows_copy(part, index).start()

        @pl.when(rows_target(index) == row)
        def _():
            rows_in[lax.rem(own_line, 2), part, own_place] = z_in[index, part]

    def forward(part):
        arrived(part_bytes.at[pl.ds(0, DEPTH - 1)], z_rsem.at[part])
        for d in DEPTH_OFFSETS:
            rows_start(part, lax.rem(col + DEPTH - d, DEPTH))

    def fwd_copy(part, lines):
        pieces = image.at[core, lax.rem(own_line + 4 - lines, 4), part]
        return pltpu.make_async_remote_copy(
            src_ref=pieces,
            dst_ref=pieces,
            send_sem=fwd_send,
            recv_sem=fwd_recv.at[part],
            device_id=(other, col),
            device_id_type=MESH,
        )

    def product_terms(side, part, first=False):
        which = core if side == 0 else 1 - core
        depth = width // PARTS
        highs, lows = [], []
        for shift in range(4):
            line = lax.rem(own_line + shift, 4)
            start = which * half + line * width + part * depth
            window = pl.ds(pl.multiple_of(start, depth), depth)
            high, low = split(image[which, line, part].reshape(depth, rank))
            right_out[window, 0:rank] = high
            right_out[window, rank : 2 * rank] = low
            right_out[window, 2 * rank : 3 * rank] = high
            highs.append(high)
            lows.append(low)
        right_high = jnp.concatenate(highs, axis=0)
        right_both = jnp.concatenate([right_high, jnp.concatenate(lows, axis=0)], axis=1)
        slots = range(4 * (1 - side), 4 * (1 - side) + 4)
        inner = pl.ds(part * depth, depth)

        def columns_of(matrix, rows):
            return jnp.concatenate([matrix[slot, rows, inner] for slot in slots], axis=1)

        for start in range(0, product.shape[0], 256):
            rows = pl.ds(start, 256)
            both = dot(columns_of(a_high, rows), right_both)
            terms = both[:, :rank] + (both[:, rank:] + dot(columns_of(a_low, rows), right_high))
            product[rows] = terms if first else product[rows] + terms

    def line_in(part, lines):
        count = 4 if lines else 3
        arrived(part_bytes.at[pl.ds(0, count)], ag_rsem.at[part, lines])
        fwd_copy(part, lines).start()

    def partner_in(part):
        arrived(part_other.at[pl.ds(0, 4 // PARTS)], fwd_recv.at[part])

    phase("z0")
    for part in range(PARTS):
        rows_start(part, col)
    forward(0)
    phase("lines0")
    for lines in (2, 1, 3, 0):
        line_in(0, lines)
    phase("product00")
    product_terms(0, 0, True)
    phase("z1")
    forward(1)
    phase("lines1")
    for lines in (2, 1, 3, 0):
        line_in(1, lines)
    phase("g_mid")
    reduce_middle(0)
    phase("product10")
    partner_in(0)
    product_terms(1, 0)
    phase("product01")
    product_terms(0, 1)
    phase("fwd_wait")
    partner_in(1)
    phase("product1")
    product_terms(1, 1)

    def rows_done(sem):
        @pl.when(has_own)
        def _():
            arrived(part_bytes.at[pl.ds(0, 7 * PARTS)], sem)

        @pl.when(jnp.logical_not(has_own))
        def _():
            arrived(part_bytes, sem)

    phase("rows_wait")
    rows_done(rows_rsem)
    phase("h_part")
    row_image = rows_in[...].reshape(8 * CHUNK, rank)
    reduce_start(1, dot_split(row_image, product[...], TN))

    row_ids = lax.broadcasted_iota(jnp.int32, (rank, rank), 0)
    col_ids = lax.broadcasted_iota(jnp.int32, (rank, rank), 1)
    identity = jnp.where(row_ids == col_ids, 1.0, 0.0).astype(F32)
    group = 4

    def lane_of(values, lane):
        return jnp.sum(
            jnp.where(col_ids[: values.shape[0]] == lane, values, 0.0), axis=1, keepdims=True
        )

    def eliminate(step, low):
        first = step * group
        pivot_rows = [table[pl.ds(first + p, 1), :] for p in range(group)]
        left_part = table[low:, :rank]
        columns = [lane_of(left_part, first + p) for p in range(group)]
        entry = {
            (p, q): lane_of(pivot_rows[p][:, :rank], first + q)
            for p in range(group)
            for q in range(p, group)
        }
        change = None
        for p in range(group):
            scale = 1.0 / entry[p, p]
            factor = jnp.where(row_ids[low:, :1] > first + p, columns[p] * scale, 0.0)
            for q in range(p + 1, group):
                columns[q] = columns[q] - factor * entry[p, q]
                weight = entry[p, q] * scale
                pivot_rows[q] = pivot_rows[q] - weight * pivot_rows[p]
                for t in range(q, group):
                    entry[q, t] = entry[q, t] - weight * entry[p, t]
            term = factor * pivot_rows[p]
            change = term if change is None else change + term
        table[low:, :] = table[low:, :] - change

    def eliminate_part(number):
        size = rank // 4
        loop(
            number * size // group,
            (number + 1) * size // group,
            functools.partial(eliminate, low=number * size),
        )

    phase("g_spread")
    reduce_spread(0)
    phase("h_mid")
    reduce_middle(1)
    phase("g_end")
    table[:, :rank] = reduce_end(0)
    table[:, rank:] = identity
    phase("elim1")
    eliminate_part(0)
    eliminate_part(1)
    phase("h_spread")
    reduce_spread(1)
    phase("elim2")
    eliminate_part(2)
    eliminate_part(3)
    pivots = jnp.sum(table[:, :rank] * identity, axis=1, keepdims=True)
    inverse = table[:, rank:] / jnp.sqrt(pivots)
    row_basis = dot_split(row_image, inverse, NT)

    phase("drain")
    arrived(part_other, half_send)
    arrived(part_other, fwd_send)
    arrived(rs_in.at[:, pl.ds(0, PLANE - 1)], rs_ssem)
    arrived(rs_in.at[:, pl.ds(0, PLANE - 1)], ag_ssem)
    arrived(rs_in.at[:, pl.ds(0, DEPTH - 1)], z_ssem)

    rows_done(rows_ssem)

    phase("h_end")
    inner = reduce_end(1)
    phase("ritz")
    raw_ritz = dot_split(dot_split(inverse, inner), inverse, NT)
    ritz = 0.5 * (raw_ritz + raw_ritz.T)
    square = dot_split(ritz, ritz) + 4.0 * penalty * identity
    frobenius = jnp.sqrt(jnp.sum(square * square, keepdims=True))

    phase("newton")
    iterate = square / frobenius
    both = iterate
    for _ in range(NS_ITERS):
        factor = 0.5 * (3.0 * identity - both)
        factor_high, factor_low = split(factor)
        factor_both = jnp.concatenate([factor_high, factor_low], axis=1)

        def scaled(left, factor_both=factor_both, factor_high=factor_high):
            high, low = split(left)
            terms = dot(high, factor_both)
            return terms[:, :rank] + (terms[:, rank:] + dot(low, factor_high))

        both = scaled(scaled(both))
        iterate = scaled(iterate)
    phase("tail")
    response = (ritz + jnp.sqrt(frobenius) * iterate) / (2.0 * penalty) - base_level * identity
    weighted_high, weighted_low = split(dot_split(row_basis, dot_split(response, inverse)))
    left_out[:, 0:rank] = weighted_high
    left_out[:, rank : 2 * rank] = weighted_high
    left_out[:, 2 * rank : 3 * rank] = weighted_low
    for which in range(2):
        pieces = 2 * (PLANE - 1) + 2 * DEPTH - 1
        arrived(product.at[pl.ds(0, 8 * pieces)], red_ssem.at[which])
    phase(None)


def solve(covariance, estimate, dual_var, start_basis):
    rows, cols = covariance.shape
    rank = start_basis.shape[1]
    vmem = pl.BlockSpec(memory_space=pltpu.VMEM)
    hbm = pl.BlockSpec(memory_space=pltpu.HBM)
    dma = pltpu.SemaphoreType.DMA
    matrix = pltpu.VMEM((8, rows, cols // 8), BF16)
    chunks = pltpu.VMEM((4, PARTS, 4, PART, rank), F32)
    pieces = pltpu.VMEM((2, PLANE, 8, rank), F32)
    return pl.pallas_call(
        solve_kernel,
        out_shape=(
            jax.ShapeDtypeStruct((rows, 3 * rank), BF16),
            jax.ShapeDtypeStruct((cols, 3 * rank), BF16),
            jax.ShapeDtypeStruct((8, rows, cols // 8), BF16),
        ),
        in_specs=[hbm, hbm, hbm, hbm],
        out_specs=(vmem, vmem, vmem),
        scratch_shapes=[
            matrix,
            matrix,
            pltpu.VMEM((rows, rank), F32),
            matrix,
            matrix,
            chunks,
            chunks,
            chunks,
            chunks,
            pltpu.VMEM((PARTS, PLANE, PART, rank), F32),
            pltpu.VMEM((2, 4, PARTS, 4, PART, rank), F32),
            pltpu.VMEM((DEPTH, PARTS, PART, rank), F32),
            pltpu.VMEM((2, PARTS, 4, PART, rank), F32),
            pltpu.VMEM((rows, rank), F32),
            pieces,
            pieces,
            pltpu.VMEM((2, 8, rank), F32),
            pieces,
            pieces,
            pltpu.VMEM((rank, 2 * rank), F32),
            dma((4,)),
            dma,
            dma,
            dma((4,)),
            dma,
            dma((PARTS,)),
            dma,
            dma((PARTS, 4)),
            dma,
            dma((PARTS,)),
            dma,
            dma((PARTS,)),
            dma,
            dma,
            dma((2,)),
            dma((2,)),
            dma((2,)),
            dma((2,)),
        ],
        compiler_params=pltpu.CompilerParams(
            collective_id=0, has_side_effects=True, vmem_limit_bytes=SOLVE_VMEM
        ),
        name="solve",
    )(covariance, estimate, dual_var, start_basis)


def finish_kernel(left, right, dual, estimate_hbm, dual_hbm, estimate_out, dual_out, out_sem):
    rows, cols = estimate_out.shape
    width = rows
    row = lax.axis_index("row")
    own_line = lax.div(row, 8)
    on_diagonal = lax.div(row, cols // rows) == lax.axis_index("col")
    row_ids = lax.broadcasted_iota(jnp.int32, (rows, width), 0)
    col_ids = lax.broadcasted_iota(jnp.int32, (rows, width), 1)

    def copies(block):
        window = pl.ds(block * width, width)
        return (
            pltpu.make_async_copy(
                estimate_out.at[:, window], estimate_hbm.at[:, window], out_sem.at[0, block]
            ),
            pltpu.make_async_copy(
                dual_out.at[:, window], dual_hbm.at[:, window], out_sem.at[1, block]
            ),
        )

    def dual_block(index):
        side = jnp.where(index // 4 == lax.rem(row, 2), 1, 0)
        return dual[4 * side + lax.rem(index + 4 - own_line, 4)]

    def tile(block):
        window = pl.ds(block * width, width)
        theta = dot(left[...], right[window, :], NT)
        level = jnp.where(
            on_diagonal & (block == lax.rem(row, cols // rows)), base_level, 0.0
        ).astype(F32)
        theta = theta + jnp.where(row_ids == col_ids, level, 0.0)
        kept = jnp.concatenate([dual_block(2 * block), dual_block(2 * block + 1)], axis=1)
        mixture = theta + kept.astype(F32)
        clipped = jnp.clip(mixture, -threshold, threshold)
        estimate_out[:, window] = mixture - clipped
        dual_out[:, window] = clipped.astype(BF16)
        for copy in copies(block):
            copy.start()

    for block in range(cols // width):
        tile(block)
    for block in range(cols // width):
        for copy in copies(block):
            copy.wait()


def finish(left, right, dual_kept):
    rows, cols = left.shape[0], right.shape[0]
    vmem = pl.BlockSpec(memory_space=pltpu.VMEM)
    hbm = pl.BlockSpec(memory_space=pltpu.HBM)
    return pl.pallas_call(
        finish_kernel,
        out_shape=(
            jax.ShapeDtypeStruct((rows, cols), F32),
            jax.ShapeDtypeStruct((rows, cols), BF16),
        ),
        in_specs=[vmem, vmem, vmem],
        out_specs=(hbm, hbm),
        scratch_shapes=[
            pltpu.VMEM((rows, cols), F32),
            pltpu.VMEM((rows, cols), BF16),
            pltpu.SemaphoreType.DMA((2, cols // rows)),
        ],
        compiler_params=pltpu.CompilerParams(vmem_limit_bytes=FINISH_VMEM),
        name="finish",
    )(left, right, dual_kept)


def body(covariance, estimate, dual_var, start_basis):
    start_basis = pltpu.with_memory_space_constraint(start_basis, pltpu.HBM)
    left, right, dual_kept = solve(covariance, estimate, dual_var, start_basis)
    return finish(left, right, dual_kept)


def solution(mesh):
    return jax.shard_map(
        body,
        mesh=mesh,
        in_specs=(P("row", "col"), P("row", "col"), P("row", "col"), P("row", None)),
        out_specs=(P("row", "col"), P("row", "col")),
        check_vma=False,
    )
```

```python
import functools

import jax
import jax.numpy as jnp
from jax import lax
from jax.experimental import pallas as pl
from jax.experimental.pallas import tpu as pltpu
from jax.sharding import PartitionSpec as P

NS_ITERS = 12
MESH = pl.DeviceIdType.MESH
F32 = jnp.float32
BF16 = jnp.bfloat16

penalty = 0.01
threshold = 0.2
base_level = 10.0
highest = lax.Precision.HIGHEST

NN = (((1,), (0,)), ((), ()))
NT = (((1,), (1,)), ((), ()))
TN = (((0,), (0,)), ((), ()))

PLANE = 16
DEPTH = 8
CHUNK = 64
PARTS = 2
PART = CHUNK // PARTS


def ring(offset, size):
    return min(offset, size - offset)


PLANE_OFFSETS = sorted(
    ((dy, dx) for dy in range(4) for dx in range(4) if dy or dx),
    key=lambda o: -(ring(o[0], 4) + ring(o[1], 4)),
)
SHIFTS = (2, 1, 3, 0)
FAR_PLANES = (3, 4, 5)
DEPTH_OFFSETS = sorted(range(1, DEPTH), key=lambda d: -ring(d, DEPTH))
COLUMN_OFFSETS = sorted(
    ((dz, dc) for dz in range(DEPTH) for dc in range(2) if dz or dc),
    key=lambda o: -(ring(o[0], DEPTH) + 0.5 * o[1]),
)
SOLVE_VMEM = 50500 * 1024
FINISH_VMEM = 32 * 1024 * 1024


def dot(left, right, dims=NN):
    return lax.dot_general(left, right, dims, preferred_element_type=F32)


def dot_full(left, right, dims=NN):
    return lax.dot_general(left, right, dims, precision=highest, preferred_element_type=F32)


def split(array):
    high = array.astype(BF16)
    return high, (array - high.astype(F32)).astype(BF16)


def dot_split(left, right, dims=NN):
    left_high, left_low = split(left)
    right_high, right_low = split(right)
    return dot(left_high, right_high, dims) + (
        dot(left_low, right_high, dims) + dot(left_high, right_low, dims)
    )


def loop(low, high, body):
    def step(index, carry):
        body(index)
        return carry

    lax.fori_loop(low, high, step, 0)


def arrived(ref, sem):
    pltpu.make_async_copy(ref, ref, sem).wait()


class Phase:
    def __init__(self):
        self.scope = None

    def __call__(self, name):
        if self.scope is not None:
            self.scope.__exit__(None, None, None)
        self.scope = None
        if name is not None:
            self.scope = jax.named_scope(name)
            self.scope.__enter__()


def solve_kernel(
    cov_hbm,
    est_hbm,
    dual_hbm,
    basis_hbm,
    left_out,
    right_out,
    dual,
    cov,
    est,
    basis,
    a_high,
    a_low,
    part_other,
    part_own,
    half_in,
    rs_send,
    rs_in,
    image,
    z_in,
    rows_in,
    product,
    red_part,
    red_in,
    red_mid,
    red_mid_in,
    red_out,
    table,
    load_sem,
    basis_sem,
    half_send,
    half_recv,
    rs_ssem,
    rs_rsem,
    ag_ssem,
    ag_rsem,
    fwd_send,
    fwd_recv,
    z_ssem,
    z_rsem,
    rows_ssem,
    rows_rsem,
    red_ssem,
    a_rsem,
    b_rsem,
    c_rsem,
):
    phase = Phase()
    phase("signal")
    row = lax.axis_index("row")
    col = lax.axis_index("col")
    core = lax.rem(row, 2)
    chip = lax.div(row, 2)
    other = row + 1 - 2 * core
    own_chunk = core * PLANE + chip
    own_line = lax.div(chip, 4)

    rank = basis.shape[1]
    width = 4 * CHUNK
    half = 4 * width

    def load(index, side, shift):
        source, target = ((cov_hbm, cov), (est_hbm, est), (dual_hbm, dual))[index]
        offset = (1 - core if side == 0 else core) * half + lax.rem(own_line + shift, 4) * width
        window = pl.ds(pl.multiple_of(offset, width), width)
        return pltpu.make_async_copy(
            source.at[:, window], target.at[4 * side + shift], load_sem.at[shift]
        )

    basis_load = pltpu.make_async_copy(basis_hbm, basis, basis_sem)
    basis_load.start()
    for shift in SHIFTS[:1]:
        for side in range(2):
            for index in range(3):
                load(index, side, shift).start()

    def plane_chip(offset):
        dy, dx = offset
        return 4 * lax.rem(own_line + dy, 4) + lax.rem(lax.rem(chip, 4) + dx, 4)

    plane_chips = [plane_chip(offset) for offset in PLANE_OFFSETS]

    def column_device(offset):
        dz, dc = offset
        return (2 * chip + lax.rem(core + dc, 2), lax.rem(col + dz, DEPTH))

    column_devices = [column_device(offset) for offset in COLUMN_OFFSETS]

    def rows_source(index):
        chunk = 8 * lax.rem(row, 4) + index
        return 2 * lax.rem(chunk, PLANE) + lax.div(chunk, PLANE)

    def rows_target(index):
        return 4 * index + lax.div(own_chunk, 8)

    barrier = pltpu.get_barrier_semaphore()

    def signal(device):
        pl.semaphore_signal(barrier, inc=1, device_id=device, device_id_type=MESH)

    for target in plane_chips:
        signal((2 * target + core, col))
    for device in column_devices:
        signal(device)

    def signal_source(index):
        source = rows_source(index)

        @pl.when(source != row)
        def _():
            signal((source, col))

    loop(0, 8, signal_source)

    has_own = lax.rem(row, 4) == lax.div(own_chunk, 8)
    peers = PLANE - 1 + 2 * DEPTH - 1 + 8 - jnp.where(has_own, 1, 0)

    for shift in SHIFTS[1:]:
        for side in range(2):
            for index in range(3):
                load(index, side, shift).start()

    phase("first")
    basis_load.wait()
    flipped = basis[...].T
    flip_high, flip_low = split(flipped)
    flip_both = jnp.concatenate([flip_high, flip_low], axis=0)

    def load_wait(shift):
        arrived(a_high.at[pl.ds(0, 6)], load_sem.at[shift])

    def partial_terms(shift):
        for side, target in ((0, part_other), (1, part_own)):
            slot = 4 * side + shift
            shifted = penalty * (est[slot].astype(F32) - dual[slot].astype(F32)) - cov[slot].astype(F32)
            high, low = split(shifted)
            a_high[slot] = high
            a_low[slot] = low
            both = dot(flip_both, high)
            terms = both[:rank] + (both[rank:] + dot(flip_high, low))
            target[shift] = terms.T.reshape(PARTS, 4, PART, rank)

    own_place = lax.rem(chip, 4)

    def half_copy(shift):
        return pltpu.make_async_remote_copy(
            src_ref=part_other.at[shift],
            dst_ref=half_in.at[shift],
            send_sem=half_send,
            recv_sem=half_recv.at[shift],
            device_id=(other, col),
            device_id_type=MESH,
        )

    def rs_copy(part, shift, place, target):
        return pltpu.make_async_remote_copy(
            src_ref=rs_send.at[shift, part, place],
            dst_ref=rs_in.at[part, chip],
            send_sem=rs_ssem,
            recv_sem=rs_rsem.at[part],
            device_id=(2 * target + core, col),
            device_id_type=MESH,
        )

    def send_terms(part, shift):
        for turn in (2, 1, 3, 0):
            if shift or turn:
                place = lax.rem(own_place + turn, 4)
                target = 4 * lax.rem(own_line + shift, 4) + place
                rs_copy(part, shift, place, target).start()

    def combine(shift):
        half_copy(shift).wait_recv()
        rs_send[shift] = part_own[shift] + half_in[shift]
        send_terms(0, shift)

    load_wait(SHIFTS[0])
    partial_terms(SHIFTS[0])
    phase("barrier")
    pl.semaphore_wait(barrier, peers)
    phase("second")
    half_copy(SHIFTS[0]).start()
    for shift in SHIFTS[1:]:
        load_wait(shift)
    for turn in range(1, 4):
        partial_terms(SHIFTS[turn])
        half_copy(SHIFTS[turn]).start()
        if turn > 1:
            combine(SHIFTS[turn - 2])
    phase("last")
    combine(SHIFTS[2])
    combine(SHIFTS[3])
    for part in range(1, PARTS):
        for shift in SHIFTS:
            send_terms(part, shift)
    def own_piece(part):
        return image.at[core, own_line, part, own_place]

    def z_copy(part, d):
        return pltpu.make_async_remote_copy(
            src_ref=own_piece(part),
            dst_ref=z_in.at[col, part],
            send_sem=z_ssem,
            recv_sem=z_rsem.at[part, 0 if d in FAR_PLANES else 1],
            device_id=(row, lax.rem(col + d, DEPTH)),
            device_id_type=MESH,
        )

    def ag_copy(part, target, lines):
        return pltpu.make_async_remote_copy(
            src_ref=own_piece(part),
            dst_ref=own_piece(part),
            send_sem=ag_ssem,
            recv_sem=ag_rsem.at[part, lines],
            device_id=(2 * target + core, col),
            device_id_type=MESH,
        )

    def a_copy(which, target):
        return pltpu.make_async_remote_copy(
            src_ref=red_part.at[which, target],
            dst_ref=red_in.at[which, chip],
            send_sem=red_ssem.at[which],
            recv_sem=a_rsem.at[which],
            device_id=(2 * target + core, col),
            device_id_type=MESH,
        )

    def b_copy(which, device):
        return pltpu.make_async_remote_copy(
            src_ref=red_mid.at[which],
            dst_ref=red_mid_in.at[which, 2 * col + core],
            send_sem=red_ssem.at[which],
            recv_sem=b_rsem.at[which],
            device_id=device,
            device_id_type=MESH,
        )

    def c_copy(which, target):
        return pltpu.make_async_remote_copy(
            src_ref=red_out.at[which, chip],
            dst_ref=red_out.at[which, chip],
            send_sem=red_ssem.at[which],
            recv_sem=c_rsem.at[which],
            device_id=(2 * target + core, col),
            device_id_type=MESH,
        )

    def reduce_start(which, value):
        red_part[which] = value.reshape(PLANE, 8, rank)
        for target in plane_chips:
            a_copy(which, target).start()
        red_in[which, chip] = red_part[which, chip]

    def reduce_middle(which):
        arrived(red_in.at[which, pl.ds(0, PLANE - 1)], a_rsem.at[which])
        piece = red_in[which, 0]
        for d in range(1, PLANE):
            piece = piece + red_in[which, d]
        red_mid[which] = piece
        red_mid_in[which, 2 * col + core] = piece
        for device in column_devices:
            b_copy(which, device).start()

    def reduce_spread(which):
        arrived(red_mid_in.at[which, pl.ds(0, 2 * DEPTH - 1)], b_rsem.at[which])
        piece = red_mid_in[which, 0]
        for d in range(1, 2 * DEPTH):
            piece = piece + red_mid_in[which, d]
        red_out[which, chip] = piece
        for target in plane_chips:
            c_copy(which, target).start()

    def reduce_end(which):
        arrived(red_out.at[which, pl.ds(0, PLANE - 1)], c_rsem.at[which])
        return red_out[which].reshape(rank, rank)

    sums = []
    for part in range(PARTS):
        phase(f"rs_wait{part}")
        arrived(rs_in.at[part, pl.ds(0, PLANE - 1)], rs_rsem.at[part])
        phase(f"spread{part}")
        rs_in[part, chip] = rs_send[0, part, own_place]
        terms = rs_in[part, 0]
        for d in range(1, PLANE):
            terms = terms + rs_in[part, d]
        image[core, own_line, part, own_place] = terms
        z_in[col, part] = terms
        sums.append(terms)
        for d in DEPTH_OFFSETS:
            z_copy(part, d).start()
        gathers = [
            ag_copy(part, target, offset[0])
            for offset, target in zip(PLANE_OFFSETS, plane_chips, strict=True)
        ]
        first = 4 if part == PARTS - 1 else PLANE
        for copy in gathers[:first]:
            copy.start()
        if part == PARTS - 1:
            total = jnp.concatenate(sums, axis=0)
            reduce_start(0, dot_full(total, total, TN))
        for copy in gathers[first:]:
            copy.start()

    part_bytes = rs_in.at[0]

    def rows_copy(part, index):
        return pltpu.make_async_remote_copy(
            src_ref=z_in.at[index, part],
            dst_ref=rows_in.at[lax.rem(own_line, 2), part, own_place],
            send_sem=rows_ssem,
            recv_sem=rows_rsem,
            device_id=(rows_target(index), col),
            device_id_type=MESH,
        )

    def rows_start(part, index):
        @pl.when(rows_target(index) != row)
        def _():
            rows_copy(part, index).start()

        @pl.when(rows_target(index) == row)
        def _():
            rows_in[lax.rem(own_line, 2), part, own_place] = z_in[index, part]

    def forward(part, far):
        planes = [d for d in DEPTH_OFFSETS if (d in FAR_PLANES) == far]
        arrived(part_bytes.at[pl.ds(0, len(planes))], z_rsem.at[part, 0 if far else 1])
        for d in planes:
            rows_start(part, lax.rem(col + DEPTH - d, DEPTH))

    def fwd_copy(part, lines):
        pieces = image.at[core, lax.rem(own_line + 4 - lines, 4), part]
        return pltpu.make_async_remote_copy(
            src_ref=pieces,
            dst_ref=pieces,
            send_sem=fwd_send,
            recv_sem=fwd_recv.at[part],
            device_id=(other, col),
            device_id_type=MESH,
        )

    def product_terms(side, part, first=False):
        which = core if side == 0 else 1 - core
        depth = width // PARTS
        highs, lows = [], []
        for shift in range(4):
            line = lax.rem(own_line + shift, 4)
            start = which * half + line * width + part * depth
            window = pl.ds(pl.multiple_of(start, depth), depth)
            high, low = split(image[which, line, part].reshape(depth, rank))
            right_out[window, 0:rank] = high
            right_out[window, rank : 2 * rank] = low
            right_out[window, 2 * rank : 3 * rank] = high
            highs.append(high)
            lows.append(low)
        right_high = jnp.concatenate(highs, axis=0)
        right_both = jnp.concatenate([right_high, jnp.concatenate(lows, axis=0)], axis=1)
        slots = range(4 * (1 - side), 4 * (1 - side) + 4)
        inner = pl.ds(part * depth, depth)

        def columns_of(matrix, rows):
            return jnp.concatenate([matrix[slot, rows, inner] for slot in slots], axis=1)

        for start in range(0, product.shape[0], 256):
            rows = pl.ds(start, 256)
            both = dot(columns_of(a_high, rows), right_both)
            terms = both[:, :rank] + (both[:, rank:] + dot(columns_of(a_low, rows), right_high))
            product[rows] = terms if first else product[rows] + terms

    def line_in(part, lines):
        count = 4 if lines else 3
        arrived(part_bytes.at[pl.ds(0, count)], ag_rsem.at[part, lines])
        fwd_copy(part, lines).start()

    def partner_in(part):
        arrived(part_other.at[pl.ds(0, 4 // PARTS)], fwd_recv.at[part])

    phase("z0")
    for part in range(PARTS):
        rows_start(part, col)
    forward(0, True)
    forward(0, False)
    phase("lines0")
    for lines in (2, 1, 3, 0):
        line_in(0, lines)
    phase("product00")
    product_terms(0, 0, True)
    phase("z1")
    forward(1, False)
    phase("z1far")
    forward(1, True)
    phase("lines1")
    for lines in (2, 1, 3, 0):
        line_in(1, lines)
    phase("g_mid")
    reduce_middle(0)
    phase("product10")
    partner_in(0)
    product_terms(1, 0)
    phase("product01")
    product_terms(0, 1)
    phase("fwd_wait")
    partner_in(1)
    phase("product1")
    product_terms(1, 1)

    def rows_done(sem):
        @pl.when(has_own)
        def _():
            arrived(part_bytes.at[pl.ds(0, 7 * PARTS)], sem)

        @pl.when(jnp.logical_not(has_own))
        def _():
            arrived(part_bytes, sem)

    phase("rows_wait")
    rows_done(rows_rsem)
    phase("h_part")
    row_image = rows_in[...].reshape(8 * CHUNK, rank)
    reduce_start(1, dot_split(row_image, product[...], TN))

    row_ids = lax.broadcasted_iota(jnp.int32, (rank, rank), 0)
    col_ids = lax.broadcasted_iota(jnp.int32, (rank, rank), 1)
    identity = jnp.where(row_ids == col_ids, 1.0, 0.0).astype(F32)
    group = 4

    def lane_of(values, lane):
        return jnp.sum(
            jnp.where(col_ids[: values.shape[0]] == lane, values, 0.0), axis=1, keepdims=True
        )

    def eliminate(step, low):
        first = step * group
        pivot_rows = [table[pl.ds(first + p, 1), :] for p in range(group)]
        left_part = table[low:, :rank]
        columns = [lane_of(left_part, first + p) for p in range(group)]
        entry = {
            (p, q): lane_of(pivot_rows[p][:, :rank], first + q)
            for p in range(group)
            for q in range(p, group)
        }
        change = None
        for p in range(group):
            scale = 1.0 / entry[p, p]
            factor = jnp.where(row_ids[low:, :1] > first + p, columns[p] * scale, 0.0)
            for q in range(p + 1, group):
                columns[q] = columns[q] - factor * entry[p, q]
                weight = entry[p, q] * scale
                pivot_rows[q] = pivot_rows[q] - weight * pivot_rows[p]
                for t in range(q, group):
                    entry[q, t] = entry[q, t] - weight * entry[p, t]
            term = factor * pivot_rows[p]
            change = term if change is None else change + term
        table[low:, :] = table[low:, :] - change

    def eliminate_part(number):
        size = rank // 4
        loop(
            number * size // group,
            (number + 1) * size // group,
            functools.partial(eliminate, low=number * size),
        )

    phase("g_spread")
    reduce_spread(0)
    phase("h_mid")
    reduce_middle(1)
    phase("g_end")
    table[:, :rank] = reduce_end(0)
    table[:, rank:] = identity
    phase("elim1")
    eliminate_part(0)
    eliminate_part(1)
    phase("h_spread")
    reduce_spread(1)
    phase("elim2")
    eliminate_part(2)
    eliminate_part(3)
    pivots = jnp.sum(table[:, :rank] * identity, axis=1, keepdims=True)
    inverse = table[:, rank:] / jnp.sqrt(pivots)
    row_basis = dot_split(row_image, inverse, NT)

    phase("drain")
    arrived(part_other, half_send)
    arrived(part_other, fwd_send)
    arrived(rs_in.at[:, pl.ds(0, PLANE - 1)], rs_ssem)
    arrived(rs_in.at[:, pl.ds(0, PLANE - 1)], ag_ssem)
    arrived(rs_in.at[:, pl.ds(0, DEPTH - 1)], z_ssem)

    rows_done(rows_ssem)

    phase("h_end")
    inner = reduce_end(1)
    phase("ritz")
    raw_ritz = dot_split(dot_split(inverse, inner), inverse, NT)
    ritz = 0.5 * (raw_ritz + raw_ritz.T)
    square = dot_split(ritz, ritz) + 4.0 * penalty * identity
    frobenius = jnp.sqrt(jnp.sum(square * square, keepdims=True))

    phase("newton")
    iterate = square / frobenius
    both = iterate
    for _ in range(NS_ITERS):
        factor = 0.5 * (3.0 * identity - both)
        factor_high, factor_low = split(factor)
        factor_both = jnp.concatenate([factor_high, factor_low], axis=1)

        def scaled(left, factor_both=factor_both, factor_high=factor_high):
            high, low = split(left)
            terms = dot(high, factor_both)
            return terms[:, :rank] + (terms[:, rank:] + dot(low, factor_high))

        both = scaled(scaled(both))
        iterate = scaled(iterate)
    phase("tail")
    response = (ritz + jnp.sqrt(frobenius) * iterate) / (2.0 * penalty) - base_level * identity
    weighted_high, weighted_low = split(dot_split(row_basis, dot_split(response, inverse)))
    left_out[:, 0:rank] = weighted_high
    left_out[:, rank : 2 * rank] = weighted_high
    left_out[:, 2 * rank : 3 * rank] = weighted_low
    for which in range(2):
        pieces = 2 * (PLANE - 1) + 2 * DEPTH - 1
        arrived(product.at[pl.ds(0, 8 * pieces)], red_ssem.at[which])
    phase(None)


def solve(covariance, estimate, dual_var, start_basis):
    rows, cols = covariance.shape
    rank = start_basis.shape[1]
    vmem = pl.BlockSpec(memory_space=pltpu.VMEM)
    hbm = pl.BlockSpec(memory_space=pltpu.HBM)
    dma = pltpu.SemaphoreType.DMA
    matrix = pltpu.VMEM((8, rows, cols // 8), BF16)
    chunks = pltpu.VMEM((4, PARTS, 4, PART, rank), F32)
    pieces = pltpu.VMEM((2, PLANE, 8, rank), F32)
    return pl.pallas_call(
        solve_kernel,
        out_shape=(
            jax.ShapeDtypeStruct((rows, 3 * rank), BF16),
            jax.ShapeDtypeStruct((cols, 3 * rank), BF16),
            jax.ShapeDtypeStruct((8, rows, cols // 8), BF16),
        ),
        in_specs=[hbm, hbm, hbm, hbm],
        out_specs=(vmem, vmem, vmem),
        scratch_shapes=[
            matrix,
            matrix,
            pltpu.VMEM((rows, rank), F32),
            matrix,
            matrix,
            chunks,
            chunks,
            chunks,
            chunks,
            pltpu.VMEM((PARTS, PLANE, PART, rank), F32),
            pltpu.VMEM((2, 4, PARTS, 4, PART, rank), F32),
            pltpu.VMEM((DEPTH, PARTS, PART, rank), F32),
            pltpu.VMEM((2, PARTS, 4, PART, rank), F32),
            pltpu.VMEM((rows, rank), F32),
            pieces,
            pieces,
            pltpu.VMEM((2, 8, rank), F32),
            pieces,
            pieces,
            pltpu.VMEM((rank, 2 * rank), F32),
            dma((4,)),
            dma,
            dma,
            dma((4,)),
            dma,
            dma((PARTS,)),
            dma,
            dma((PARTS, 4)),
            dma,
            dma((PARTS,)),
            dma,
            dma((PARTS, 2)),
            dma,
            dma,
            dma((2,)),
            dma((2,)),
            dma((2,)),
            dma((2,)),
        ],
        compiler_params=pltpu.CompilerParams(
            collective_id=0, has_side_effects=True, vmem_limit_bytes=SOLVE_VMEM
        ),
        name="solve",
    )(covariance, estimate, dual_var, start_basis)


def finish_kernel(left, right, dual, estimate_hbm, dual_hbm, estimate_out, dual_out, out_sem):
    rows, cols = estimate_out.shape
    narrow = cols // 8
    blocks = [(0, narrow), (narrow, narrow)] + [
        (start, 2 * narrow) for start in range(2 * narrow, cols, 2 * narrow)
    ]
    row = lax.axis_index("row")
    own_line = lax.div(row, 8)
    shift = row * rows - lax.axis_index("col") * cols

    def copies(index):
        window = pl.ds(*blocks[index])
        return (
            pltpu.make_async_copy(
                estimate_out.at[:, window], estimate_hbm.at[:, window], out_sem.at[0, index]
            ),
            pltpu.make_async_copy(
                dual_out.at[:, window], dual_hbm.at[:, window], out_sem.at[1, index]
            ),
        )

    def dual_block(index):
        side = jnp.where(index // 4 == lax.rem(row, 2), 1, 0)
        return dual[4 * side + lax.rem(index + 4 - own_line, 4)]

    def tile(index):
        start, width = blocks[index]
        window = pl.ds(start, width)
        theta = dot(left[...], right[window, :], NT)
        offsets = lax.broadcasted_iota(jnp.int32, (rows, width), 1) - lax.broadcasted_iota(
            jnp.int32, (rows, width), 0
        )
        theta = theta + jnp.where(offsets == shift - start, base_level, 0.0).astype(F32)
        kept = [dual_block(n) for n in range(start // narrow, (start + width) // narrow)]
        mixture = theta + jnp.concatenate(kept, axis=1).astype(F32)
        clipped = jnp.clip(mixture, -threshold, threshold)
        estimate_out[:, window] = mixture - clipped
        dual_out[:, window] = clipped.astype(BF16)
        for copy in copies(index):
            copy.start()

    for index in range(len(blocks)):
        tile(index)
    for index in range(len(blocks)):
        for copy in copies(index):
            copy.wait()


def finish(left, right, dual_kept):
    rows, cols = left.shape[0], right.shape[0]
    vmem = pl.BlockSpec(memory_space=pltpu.VMEM)
    hbm = pl.BlockSpec(memory_space=pltpu.HBM)
    return pl.pallas_call(
        finish_kernel,
        out_shape=(
            jax.ShapeDtypeStruct((rows, cols), F32),
            jax.ShapeDtypeStruct((rows, cols), BF16),
        ),
        in_specs=[vmem, vmem, vmem],
        out_specs=(hbm, hbm),
        scratch_shapes=[
            pltpu.VMEM((rows, cols), F32),
            pltpu.VMEM((rows, cols), BF16),
            pltpu.SemaphoreType.DMA((2, 5)),
        ],
        compiler_params=pltpu.CompilerParams(vmem_limit_bytes=FINISH_VMEM),
        name="finish",
    )(left, right, dual_kept)


def body(covariance, estimate, dual_var, start_basis):
    start_basis = pltpu.with_memory_space_constraint(start_basis, pltpu.HBM)
    left, right, dual_kept = solve(covariance, estimate, dual_var, start_basis)
    return finish(left, right, dual_kept)


def solution(mesh):
    return jax.shard_map(
        body,
        mesh=mesh,
        in_specs=(P("row", "col"), P("row", "col"), P("row", "col"), P("row", None)),
        out_specs=(P("row", "col"), P("row", "col")),
        check_vma=False,
    )
```
